32 devices in a mesh: ctx: 8 (over y, x, core), exp: 4 (over z).
Axes of the slice: x: 2, y: 2, z: 4, core: 2. Of those that a mesh axis runs over, the one named last changes fastest.
Arguments:
- hidden_in: bfloat16 [1024, 4096], P('ctx', 'exp'), may hold values from -6 to 6
- query_vectors: bfloat16 [1024, 2048], P('ctx', 'exp'), may hold values from -6 to 6
- key_vectors: bfloat16 [1024, 2048], P('ctx', 'exp'), may hold values from -6 to 6
- value_vectors: bfloat16 [1024, 2048], P('ctx', 'exp'), may hold values from -24 to 24
- out_weight: bfloat16 [2048, 4096], P('exp'), may hold values from -0.125 to 0.125
- norm_gain: float32 [4096], replicated, may hold values from 0.5 to 1.5
- gate_proj: bfloat16 [4, 4096, 11008], P('exp', None, 'ctx'), may hold values from -0.09375 to 0.09375
- up_proj: bfloat16 [4, 4096, 11008], P('exp', None, 'ctx'), may hold values from -0.09375 to 0.09375
- down_proj: bfloat16 [4, 11008, 4096], P('exp', 'ctx'), may hold values from -0.0546875 to 0.0546875
- expert_ids: int32 [1024, 2], P('ctx'), may hold values from 0 to 3, all different within a row; in each aligned block of 128 rows (0 to 127, 128 to 255, ...) at most 80 rows name the same one
- gate_scale: float32 [1024, 2], P('ctx'), may hold values from 0.1 to 1
Outputs:
- layer_out: bfloat16 [1024, 4096], P('ctx', 'exp')
The draws below stay inside these ranges and needn't reach their ends.
Inputs may be any that keep to these rules, and one draw needn't show every extreme that they name: `expert_ids`: each row names two different experts. In each aligned block of 128 rows (the rows of one ctx device) no expert is named by more than 80 rows, and in some blocks some expert is named by exactly 80 rows.
All inputs are finite; a program needn't handle non-finite values.
Results may differ from the reference program's by a relative error of at most 0.017.
Values may be sent and summed in bfloat16 or wider, within the bound.
A program may use at most 128 MiB of HBM per device.

```python
import math
import jax
import jax.numpy as jnp
import numpy as np
from jax import lax

D = 4096
HEADS = 16
HEAD_DIM = 128
FF = 11008
TOK_DEV = 128
TOKENS = 1024
EXPERTS = 4
CAP = 80
N_CTX = 8


def draw_pair(key):
    shape = (TOKENS, HEADS * HEAD_DIM)
    first = jnp.clip(jax.random.normal(jax.random.fold_in(key, 11), shape, jnp.float32), -6.0, 6.0)
    second = jnp.clip(jax.random.normal(jax.random.fold_in(key, 12), shape, jnp.float32), -6.0, 6.0)
    return (first, second)


def draw_query_vectors(key, part):
    return draw_pair(key)[0].astype(jnp.bfloat16)


def draw_key_vectors(key, part):
    return draw_pair(key)[1].astype(jnp.bfloat16)


def draw_hidden_in(key, part):
    shape = (TOKENS, D)
    log_scale = jax.random.uniform(jax.random.fold_in(key, 21), (TOKENS, 1), jnp.float32, jnp.log(0.3), jnp.log(1.5))
    row_scale = jnp.exp(log_scale)
    fraction = jnp.arange(D, dtype=jnp.float32)[None, :] / (D - 1)
    column_scale = jnp.exp(jnp.log(0.4) + fraction * (jnp.log(2.0) - jnp.log(0.4)))
    entries = jax.random.normal(jax.random.fold_in(key, 22), shape, jnp.float32)
    return jnp.clip(entries * row_scale * column_scale, -6.0, 6.0).astype(jnp.bfloat16)


def shard_levels(stream_key, shape, shards, least, largest):
    def one(position, parts):
        draws = jax.random.uniform(jax.random.fold_in(jax.random.fold_in(stream_key, 6), position), (parts,), jnp.float32, least / len(shards), largest / len(shards))
        return jnp.repeat(jnp.exp(draws), shape[position] // parts).reshape((-1,) + (1,) * (len(shape) - position - 1))

    loudness = one(*shards[0])
    for cut in shards[1:]:
        loudness = loudness * one(*cut)
    return loudness


def assign_block(own_key, own, number, rows, count, top, most, lean):
    order = jax.random.permutation(own_key, count)
    heavy_load, ordinary = portions_of(count, rows * top, most, lean, True), portions_of(count, rows * top, most, lean, False)
    places = jnp.arange(count)

    def named(tallies, offset_by):
        used = int((tallies > 0).sum())
        fixed = max(1, used // 4)
        shifted = fixed + (places - fixed + offset_by * (used - fixed)) % max(1, count - fixed)
        return jnp.zeros((count,), jnp.int32).at[order[jnp.where(places < fixed, places, shifted)]].set(jnp.asarray(tallies, jnp.int32))

    tallies = jnp.where(number % 4 == 0, named(heavy_load, number // 4), named(ordinary, number - number // 4 - 1))
    mixed = jax.random.permutation(jax.random.fold_in(own, 3), count)
    donor, taker = mixed[0:count // 2 * 2:2], mixed[1:count // 2 * 2:2]
    slack = jnp.minimum(tallies[donor] - 1, most - tallies[taker]) // 2
    slack = jnp.where((donor == order[0]) | (taker == order[0]) | (tallies[taker] == 0), 0, jnp.maximum(slack, 0))
    shifted = jax.random.randint(jax.random.fold_in(own, 4), (count // 2,), 0, 1 << 20) % (slack + 1)
    tallies = tallies.at[donor].add(-shifted).at[taker].add(shifted)
    members = jnp.searchsorted(jnp.cumsum(tallies), jnp.arange(rows * top), side="right").astype(jnp.int32)
    grid = members.reshape(top, rows).T
    grid = grid[jax.random.permutation(jax.random.fold_in(own, 1), rows)]
    offset_by = jax.random.randint(jax.random.fold_in(own, 2), (rows, 1), 0, top)
    return jnp.take_along_axis(grid, (jnp.arange(top)[None, :] + offset_by) % top, axis=1)


def portions_of(number_of, total, limit, skew, full):
    weights = [(1 << 20) // math.isqrt(grade ** skew) + 1 for grade in range(1, number_of + 1)]
    largest = limit if full else min(limit, max(-(-total // number_of), total * weights[0] // sum(weights)))
    least = 1 if total - largest >= number_of - 1 else 0
    given, rest = [largest] + [least] * (number_of - 1), total - largest - least * (number_of - 1)
    while rest > 0:
        free = [i for i in range(1, number_of) if given[i] < largest] or [i for i in range(1, number_of) if given[i] < limit]
        whole, left = sum([weights[i] for i in free]), rest
        for i in free:
            extra = min(limit - given[i], max(1, left * weights[i] // whole), rest)
            given[i] = given[i] + extra
            rest = rest - extra
    return np.array(given)


def gaussian(rng, dims, width, bound, cuts=(), held_as=jnp.bfloat16):
    values = jax.random.normal(rng, dims, jnp.float32) * width
    if len(cuts) > 0:
        values = shard_levels(rng, dims, cuts, -0.22, 0.18) * values
    return jnp.clip(values, min=-bound, max=bound).astype(held_as)


def setup_inputs(seed: int = 0) -> dict:
    key_of = jax.random.split(jax.random.key(seed), 12)
    hidden_in = draw_hidden_in(jax.random.fold_in(key_of[11], 71), 0)
    query_vectors = draw_query_vectors(jax.random.fold_in(key_of[11], 71), 0)
    key_vectors = draw_key_vectors(jax.random.fold_in(key_of[11], 71), 0)
    value_vectors = gaussian(key_of[3], (TOKENS, HEADS * HEAD_DIM), 4.0, 24.0, ((0, 8), (1, 4)))
    out_weight = gaussian(key_of[4], (HEADS * HEAD_DIM, D), (HEADS * HEAD_DIM) ** -0.5, 0.125, ((0, 4),))
    norm_gain = jnp.clip(1.0 + 0.1 * jax.random.normal(key_of[5], (D,), jnp.float32), 0.5, 1.5)
    gate_proj = gaussian(key_of[6], (EXPERTS, D, FF), D ** -0.5, 0.09375, ((0, 4), (2, 8)))
    up_proj = gaussian(key_of[7], (EXPERTS, D, FF), D ** -0.5, 0.09375, ((0, 4), (2, 8)))
    down_proj = gaussian(key_of[8], (EXPERTS, FF, D), FF ** -0.5, 0.0546875, ((0, 4), (1, 8)))
    expert_ids_keys = jax.random.split(jax.random.fold_in(key_of[9], 1), TOKENS // TOK_DEV)
    expert_ids_turns = jax.random.permutation(jax.random.fold_in(key_of[9], 3), TOKENS // TOK_DEV)
    expert_ids = jax.vmap(lambda own, number: assign_block(jax.random.fold_in(key_of[9], 2), own, number, TOK_DEV, EXPERTS, 2, CAP, 2))(expert_ids_keys, expert_ids_turns).reshape((TOKENS, 2))
    gate_scale = jnp.clip(0.1 + 0.9 * jax.random.uniform(key_of[10], (TOKENS, 2), jnp.float32) ** shard_levels(key_of[10], (TOKENS, 2), ((0, 8),), -0.2, 0.2), 0.1, 1.0)
    return dict(hidden_in=hidden_in, query_vectors=query_vectors, key_vectors=key_vectors, value_vectors=value_vectors, out_weight=out_weight, norm_gain=norm_gain, gate_proj=gate_proj, up_proj=up_proj, down_proj=down_proj, expert_ids=expert_ids, gate_scale=gate_scale)


epsilon = 1e-05

def attend_head(query_head, key_head, value_head):
    scores = jnp.dot(query_head, key_head.T, preferred_element_type=jnp.float32) * HEAD_DIM ** (-0.5)
    row_pos = lax.broadcasted_iota(jnp.int32, scores.shape, 0)
    col_pos = lax.broadcasted_iota(jnp.int32, scores.shape, 1)
    visible = col_pos <= row_pos
    scores = jnp.where(visible, scores, -1e+30)
    row_max = lax.optimization_barrier(jnp.max(scores, axis=1, keepdims=True))
    weights = jnp.where(visible, jnp.exp(scores - row_max), 0.0)
    denominator = lax.optimization_barrier(jnp.sum(weights, axis=1, keepdims=True))
    head_out = jnp.dot(weights.astype(jnp.bfloat16), value_head, preferred_element_type=jnp.float32)
    return head_out / denominator

def reference(hidden_in, query_vectors, key_vectors, value_vectors, out_weight, norm_gain, gate_proj, up_proj, down_proj, expert_ids, gate_scale):
    query_split = query_vectors.reshape(TOKENS, HEADS, HEAD_DIM).transpose(1, 0, 2)
    key_split = key_vectors.reshape(TOKENS, HEADS, HEAD_DIM).transpose(1, 0, 2)
    value_split = value_vectors.reshape(TOKENS, HEADS, HEAD_DIM).transpose(1, 0, 2)
    attended = lax.map(lambda triple: attend_head(triple[0], triple[1], triple[2]), (query_split, key_split, value_split))
    attended = attended.transpose(1, 0, 2).reshape(TOKENS, HEADS * HEAD_DIM).astype(jnp.bfloat16)
    projected = jnp.dot(attended, out_weight, preferred_element_type=jnp.float32)
    residual = (hidden_in.astype(jnp.float32) + projected).astype(jnp.bfloat16)
    residual_wide = residual.astype(jnp.float32)
    inverse = lax.rsqrt(lax.optimization_barrier(jnp.mean(residual_wide * residual_wide, axis=1, keepdims=True)) + epsilon)
    normed = (residual_wide * inverse * norm_gain.astype(jnp.float32)[None, :]).astype(jnp.bfloat16)
    block_ids = expert_ids.reshape(N_CTX, TOK_DEV * 2)
    onehot = (block_ids[:, :, None] == jnp.arange(EXPERTS, dtype=jnp.int32)[None, None, :]).astype(jnp.int32)
    earlier = jnp.cumsum(onehot, axis=1) - onehot
    slot_index = lax.optimization_barrier(jnp.sum(earlier * onehot, axis=2))
    slot_row = (jnp.arange(N_CTX, dtype=jnp.int32)[:, None] * CAP + slot_index).reshape(-1).astype(jnp.int32)
    flat_ids = expert_ids.reshape(-1)
    source = jnp.repeat(normed, 2, axis=0)
    rows_all = N_CTX * CAP
    group_width = FF // N_CTX

    def per_expert(running, expert_index):
        target = jnp.where(flat_ids == expert_index, slot_row, rows_all).astype(jnp.int32)
        buffer = jnp.zeros((rows_all, D), jnp.bfloat16).at[target].set(source, mode='drop')
        gate_act = jnp.dot(buffer, gate_proj[expert_index], preferred_element_type=jnp.float32)
        up_act = jnp.dot(buffer, up_proj[expert_index], preferred_element_type=jnp.float32)
        hidden = (jax.nn.silu(gate_act) * up_act).astype(jnp.bfloat16)
        down_one = down_proj[expert_index]

        def add_group(group_index, summed):
            piece_in = lax.dynamic_slice_in_dim(hidden, group_index * group_width, group_width, 1)
            piece_weight = lax.dynamic_slice_in_dim(down_one, group_index * group_width, group_width, 0)
            piece_out = jnp.dot(piece_in, piece_weight, preferred_element_type=jnp.float32).astype(jnp.bfloat16)
            piece_out = lax.optimization_barrier(piece_out)
            return summed + piece_out.astype(jnp.float32)
        expert_out = lax.fori_loop(0, N_CTX, add_group, jnp.zeros((rows_all, D), jnp.float32)).astype(jnp.bfloat16)
        picked = expert_out[jnp.clip(slot_row, 0, rows_all - 1)]
        running = running + jnp.where((flat_ids == expert_index)[:, None], picked.astype(jnp.float32), 0.0)
        return (running, None)
    gathered, _ = lax.scan(per_expert, jnp.zeros((TOKENS * 2, D), jnp.float32), jnp.arange(EXPERTS, dtype=jnp.int32))
    gathered = gathered.reshape(TOKENS, 2, D)
    layer_out = residual_wide + gate_scale[:, 0:1] * gathered[:, 0] + gate_scale[:, 1:2] * gathered[:, 1]
    return layer_out.astype(jnp.bfloat16)
```

```python
import functools

import jax
import jax.numpy as jnp
from jax import lax
from jax.experimental import pallas as pl
from jax.experimental.pallas import tpu as pltpu
from jax.sharding import PartitionSpec as P

HEAD_DIM = 128
MESH = pl.DeviceIdType.MESH

epsilon = 1e-05
masked_score = -1e30
PIECES = 4


def mixed(index, flip):
    result = index
    bit = 1
    while bit <= flip:
        if flip & bit:
            result = result + bit - 2 * bit * ((index // bit) % 2)
        bit *= 2
    return result


def remote(src, dst, send_sem, recv_sem, device):
    return pltpu.make_async_remote_copy(
        src_ref=src, dst_ref=dst, send_sem=send_sem, recv_sem=recv_sem,
        device_id=device, device_id_type=MESH,
    )


def greet(devices):
    barrier = pltpu.get_barrier_semaphore()
    for device in devices:
        pl.semaphore_signal(barrier, inc=1, device_id=device, device_id_type=MESH)
    pl.semaphore_wait(barrier, len(devices))


def gather_kernel(chips, k_ref, v_ref, ko_ref, vo_ref, local_sem, send_sem, pass_sem, recv_sem, half_send, half_recv):
    ctx, exp = lax.axis_index("ctx"), lax.axis_index("exp")
    chip, core = ctx // 2, ctx % 2
    rows = k_ref.shape[0]
    partner = (chip * 2 + 1 - core, exp)
    others = [(((chip + j) % chips) * 2 + core, exp) for j in range(1, chips)]
    pairs = ((k_ref, ko_ref), (v_ref, vo_ref))
    width = k_ref.shape[1]
    square = chips == 4
    near = (1, 2) if square else tuple(range(chips - 1, 0, -1))

    def device_of(j):
        return (mixed(chip, j) * 2 + core, exp) if square else others[j - 1]

    def source_of(j):
        return mixed(chip, j) if square else (chip + chips - j) % chips

    def half(ref, owner, which):
        part = pl.ds(pl.multiple_of(owner * rows, rows), rows)
        return ref.at[part, pl.ds(which * (width // 2), width // 2)]

    def block(ref, owner):
        return ref.at[pl.ds(pl.multiple_of(owner * rows, rows), rows), :]

    own = []
    for i, (src, dst) in enumerate(pairs):
        own.append(pltpu.make_async_copy(src, block(dst, ctx), local_sem.at[i]))
        own[-1].start()
    greet([partner] + others)
    sent = []
    for i, (src, dst) in enumerate(pairs):
        for j in near:
            sent.append(remote(src, block(dst, ctx), send_sem.at[i, j], recv_sem.at[i, ctx], device_of(j)))
            sent[-1].start()
        sent.append(remote(src, block(dst, ctx), send_sem.at[i, 0], recv_sem.at[i, ctx], partner))
        sent[-1].start()
    for i, (src, dst) in enumerate(pairs):
        for j in near:
            owner = source_of(j) * 2 + core
            here = block(dst, owner)
            passed = remote(here, here, pass_sem.at[i, j], recv_sem.at[i, owner], partner)
            passed.wait_recv()
            if square:
                piece = half(dst, owner, j - 1)
                sent.append(remote(piece, piece, half_send.at[i, j - 1], half_recv.at[i, j - 1], device_of(3 - j)))
                sent[-1].start()
            passed.start()
            sent.append(passed)
    for i, (src, dst) in enumerate(pairs):
        if square:
            owner = mixed(chip, 3) * 2 + core
            for h in range(2):
                piece = half(dst, owner, h)
                remote(piece, piece, half_send.at[i, h], half_recv.at[i, h], partner).wait_recv()
            here = block(dst, owner)
            sent.append(remote(here, here, pass_sem.at[i, 3], recv_sem.at[i, owner], partner))
            sent[-1].start()
    for i, (src, dst) in enumerate(pairs):
        for j in range(chips):
            owner = ((chip + chips - j) % chips) * 2 + 1 - core
            here = block(dst, owner)
            remote(here, here, pass_sem.at[i, 0], recv_sem.at[i, owner], partner).wait_recv()
    for copy in sent:
        copy.wait_send()
    for copy in own:
        copy.wait()


def gather_blocks(chips, keys, values):
    rows, width = keys.shape
    whole = jax.ShapeDtypeStruct((rows * chips * 2, width), keys.dtype)
    return pl.pallas_call(
        functools.partial(gather_kernel, chips),
        out_shape=(whole, whole),
        in_specs=[pl.BlockSpec(memory_space=pltpu.VMEM)] * 2,
        out_specs=[pl.BlockSpec(memory_space=pltpu.VMEM)] * 2,
        scratch_shapes=[
            pltpu.SemaphoreType.DMA((2,)),
            pltpu.SemaphoreType.DMA((2, chips)),
            pltpu.SemaphoreType.DMA((2, chips)),
            pltpu.SemaphoreType.DMA((2, chips * 2)),
            pltpu.SemaphoreType.DMA((2, 2)),
            pltpu.SemaphoreType.DMA((2, 2)),
        ],
        compiler_params=pltpu.CompilerParams(collective_id=0, has_side_effects=True),
        name="gather_blocks",
    )(keys, values)


def project_kernel(experts, att_ref, weight_ref, hidden_ref, out_ref, terms, landed, send_sem, recv_sem):
    ctx, exp = lax.axis_index("ctx"), lax.axis_index("exp")
    width = hidden_ref.shape[1]
    levels = experts.bit_length() - 1
    depth = hidden_ref.shape[0] // PIECES
    peers = [(ctx, mixed(exp, 1 << b)) for b in range(levels)]
    greet(peers)
    sent = []

    def slot(level, k):
        return sum(experts >> (b + 1) for b in range(level)) + k // (2 << level)

    def send(level, k, piece):
        to = slot(level, k - (1 << level))
        here = pl.ds(piece * depth, depth)
        sent.append(remote(
            terms.at[k, here], landed.at[to, here], send_sem.at[to, piece], recv_sem.at[to, piece], peers[level]
        ))
        sent[-1].start()

    order = [k for k in range(experts - 1, -1, -1) if k % 2] + [k for k in range(experts - 1, -1, -1) if not k % 2]
    for k in order:
        columns = pl.ds(pl.multiple_of(mixed(exp, k) * width, width), width)
        terms[k] = jnp.dot(
            att_ref[...], weight_ref[:, columns], preferred_element_type=jnp.float32
        ).astype(jnp.bfloat16)
        if k % 2:
            for piece in range(PIECES):
                send(0, k, piece)
    for level in range(levels):
        for k in range(experts - (2 << level), -1, -(2 << level)):
            at = slot(level, k)
            for piece in range(PIECES):
                here = pl.ds(piece * depth, depth)
                view = landed.at[at, here]
                remote(view, view, send_sem.at[at, piece], recv_sem.at[at, piece], peers[level]).wait_recv()
                total = terms[k, here, :].astype(jnp.float32) + landed[at, here, :].astype(jnp.float32)
                if level + 1 < levels:
                    terms[k, here, :] = total.astype(jnp.bfloat16)
                    if k & (2 << level):
                        send(level + 1, k, piece)
                else:
                    out_ref[here, :] = (hidden_ref[here, :].astype(jnp.float32) + total).astype(jnp.bfloat16)
    for copy in sent:
        copy.wait_send()


def project(experts, attended, weight, hidden):
    rows, width = hidden.shape
    return pl.pallas_call(
        functools.partial(project_kernel, experts),
        out_shape=jax.ShapeDtypeStruct((rows, width), jnp.bfloat16),
        in_specs=[pl.BlockSpec(memory_space=pltpu.VMEM)] * 3,
        out_specs=pl.BlockSpec(memory_space=pltpu.VMEM),
        scratch_shapes=[
            pltpu.VMEM((experts, rows, width), jnp.bfloat16),
            pltpu.VMEM((experts - 1, rows, width), jnp.bfloat16),
            pltpu.SemaphoreType.DMA((experts - 1, PIECES)),
            pltpu.SemaphoreType.DMA((experts - 1, PIECES)),
        ],
        compiler_params=pltpu.CompilerParams(
            collective_id=1, has_side_effects=True, vmem_limit_bytes=32 * 1024 * 1024
        ),
        name="project_reduce",
    )(attended, weight, hidden)


def tiles(width, body, size=256):
    full = width // size
    if full:
        @pl.loop(0, full)
        def _(t):
            body(pl.ds(pl.multiple_of(t * size, size), size))
    if width % size:
        body(pl.ds(full * size, width % size))


def times_transposed(left, right):
    return lax.dot_general(
        left, right, (((1,), (1,)), ((), ())), preferred_element_type=jnp.float32
    )


def experts_kernel(
    chips, experts, buf, gain, gate_hbm, up_hbm, down_hbm, out,
    rows_all, wg, wu, wd, acc_g, acc_u, scaled, hidden, squares, pair_in, chip_in, final,
    w_sem, local_sem, a2a_send, ag_send, pass_send, ag_recv,
    pair_send, pair_recv, rs_send, rs_recv, ret_send, ret_recv,
):
    ctx, exp = lax.axis_index("ctx"), lax.axis_index("exp")
    chip, core = ctx // 2, ctx % 2
    cap, width = buf.shape[1:]
    total_rows = chips * 2 * cap
    features = gate_hbm.shape[2]
    inner = gate_hbm.shape[1]
    partner = (chip * 2 + 1 - core, exp)
    others = [(((chip + j) % chips) * 2 + core, exp) for j in range(1, chips)]
    peers = [(ctx, mixed(exp, k)) for k in range(1, experts)]

    loads = []
    for k in range(experts):
        part = pl.ds(pl.multiple_of(mixed(exp, k) * width, width), width)
        loads.append((
            pltpu.make_async_copy(gate_hbm.at[0, :, part], wg.at[k], w_sem.at[0, k]),
            pltpu.make_async_copy(up_hbm.at[0, :, part], wu.at[k], w_sem.at[1, k]),
        ))
    downs = []
    for k in range(experts):
        part = pl.ds(pl.multiple_of(mixed(exp, k) * width, width), width)
        downs.append(pltpu.make_async_copy(down_hbm.at[0, :, part], wd.at[k], w_sem.at[2, k]))

    def span(index):
        return pl.ds(pl.multiple_of(index * cap, cap), cap)

    mine = core * chips + chip

    own = pltpu.make_async_copy(buf.at[0], rows_all.at[0, span(mine), :], local_sem.at[0])
    own.start()
    for gate_load, up_load in loads:
        gate_load.start()
        up_load.start()
    for k in range(experts - 1, -1, -1):
        downs[k].start()
    greet([partner] + others + peers)

    sent = []
    for k in range(1, experts):
        copy = remote(buf.at[k], rows_all.at[k, span(mine), :], a2a_send.at[k], ag_recv.at[k, mine], peers[k - 1])
        copy.start()
        sent.append(copy)

    def spread(k):
        here = rows_all.at[k, span(mine), :]
        if k == 0:
            own.wait()
        else:
            remote(here, here, a2a_send.at[k], ag_recv.at[k, mine], partner).wait_recv()
        for j in range(chips - 1, 0, -1):
            copy = remote(here, here, ag_send.at[k, j], ag_recv.at[k, mine], others[j - 1])
            copy.start()
            sent.append(copy)
        copy = remote(here, here, ag_send.at[k, 0], ag_recv.at[k, mine], partner)
        copy.start()
        sent.append(copy)

    def collect(k):
        for j in range(1, chips):
            owner = core * chips + (chip + chips - j) % chips
            here = rows_all.at[k, span(owner), :]
            copy = remote(here, here, pass_send.at[k, j], ag_recv.at[k, owner], partner)
            copy.wait_recv()
            copy.start()
            sent.append(copy)
        for j in range(chips):
            owner = (1 - core) * chips + (chip + chips - j) % chips
            here = rows_all.at[k, span(owner), :]
            remote(here, here, pass_send.at[k, 0], ag_recv.at[k, owner], partner).wait_recv()

    spread(0)
    spread(1)
    for k in range(experts):
        collect(k)
        if k + 2 < experts:
            spread(k + 2)
        gain_row = gain[mixed(exp, k)]

        @pl.loop(0, chips * 2)
        def _(b, k=k, gain_row=gain_row):
            x = rows_all[k, span(b), :].astype(jnp.float32)
            square = jnp.broadcast_to(jnp.sum(x * x, axis=1, keepdims=True), (cap, 128))
            squares[span(b), :] = square if k == 0 else squares[span(b), :] + square
            scaled[span(b), :] = (x * gain_row).astype(jnp.bfloat16)

        loads[k][0].wait()
        loads[k][1].wait()
        last = k == experts - 1
        if last:
            squares[...] = lax.rsqrt(squares[...] * (1.0 / features) + epsilon)

        def up_tile(cols, k=k, last=last):
            g = times_transposed(scaled[...], wg[k, cols, :])
            u = times_transposed(scaled[...], wu[k, cols, :])
            if k:
                g = g + acc_g[:, cols]
                u = u + acc_u[:, cols]
            if last:
                inverse = squares[:, 0:1]
                g = g * inverse
                u = u * inverse
                hidden[:, cols] = (g / (1.0 + jnp.exp(-g)) * u).astype(jnp.bfloat16)
            else:
                acc_g[:, cols] = g
                acc_u[:, cols] = u

        tiles(inner, up_tile)

    for copy in sent:
        copy.wait_send()
    sent = []
    half = chips * cap

    def half_of(which):
        return pl.ds(pl.multiple_of(which * half, half), half)

    def multiply(k):
        downs[k].wait()

        def down_tile(cols):
            rows_all[k, :, cols] = jnp.dot(
                hidden[...], wd[k, :, cols], preferred_element_type=jnp.float32
            ).astype(jnp.bfloat16)

        tiles(width, down_tile)
        copy = remote(rows_all.at[k, half_of(1 - core), :], pair_in.at[k], pair_send.at[k], pair_recv.at[k], partner)
        copy.start()
        sent.append(copy)

    def merge(k):
        remote(pair_in.at[k], pair_in.at[k], pair_send.at[k], pair_recv.at[k], partner).wait_recv()
        for j in range(chips - 1, -1, -1):
            to = (chip + j) % chips
            place = span(core * chips + to)
            rows_all[k, place, :] = (
                rows_all[k, place, :].astype(jnp.float32) + pair_in[k, span(to), :].astype(jnp.float32)
            ).astype(jnp.bfloat16)
            if j:
                copy = remote(rows_all.at[k, place, :], chip_in.at[k, j - 1], rs_send.at[k, j], rs_recv.at[k, j], others[j - 1])
                copy.start()
                sent.append(copy)

    def finish(k):
        value = rows_all[k, span(mine), :].astype(jnp.float32)
        for j in range(1, chips):
            here = chip_in.at[k, j - 1]
            remote(here, here, rs_send.at[k, j], rs_recv.at[k, j], partner).wait_recv()
            value = value + chip_in[k, j - 1].astype(jnp.float32)
        if k == 0:
            out[0] = value.astype(jnp.bfloat16)
        else:
            final[k] = value.astype(jnp.bfloat16)
            copy = remote(final.at[k], out.at[k], ret_send.at[k], ret_recv.at[k], peers[k - 1])
            copy.start()
            sent.append(copy)

    order = list(range(experts - 1, -1, -1))
    for step in range(experts + 2):
        if step < experts:
            multiply(order[step])
        if 1 <= step <= experts:
            merge(order[step - 1])
        if step >= 2:
            finish(order[step - 2])
    for k in range(1, experts):
        remote(out.at[k], out.at[k], ret_send.at[k], ret_recv.at[k], peers[k - 1]).wait_recv()
    for copy in sent:
        copy.wait_send()


def run_experts(chips, experts, buffer, gain, gate, up, down):
    _, cap, width = buffer.shape
    inner = gate.shape[1]
    rows = chips * 2 * cap
    bf16, f32 = jnp.bfloat16, jnp.float32
    dma = pltpu.SemaphoreType.DMA
    vmem = pl.BlockSpec(memory_space=pltpu.VMEM)
    hbm = pl.BlockSpec(memory_space=pl.ANY)
    return pl.pallas_call(
        functools.partial(experts_kernel, chips, experts),
        out_shape=jax.ShapeDtypeStruct((experts, cap, width), bf16),
        in_specs=[vmem, vmem, hbm, hbm, hbm],
        out_specs=vmem,
        scratch_shapes=[
            pltpu.VMEM((experts, rows, width), bf16),
            pltpu.VMEM((experts, inner, width), bf16),
            pltpu.VMEM((experts, inner, width), bf16),
            pltpu.VMEM((experts, inner, width), bf16),
            pltpu.VMEM((rows, inner), f32),
            pltpu.VMEM((rows, inner), f32),
            pltpu.VMEM((rows, width), bf16),
            pltpu.VMEM((rows, inner), bf16),
            pltpu.VMEM((rows, 128), f32),
            pltpu.VMEM((experts, chips * cap, width), bf16),
            pltpu.VMEM((experts, chips - 1, cap, width), bf16),
            pltpu.VMEM((experts, cap, width), bf16),
            dma((3, experts)),
            dma((1,)),
            dma((experts,)),
            dma((experts, chips)),
            dma((experts, chips)),
            dma((experts, chips * 2)),
            dma((experts,)),
            dma((experts,)),
            dma((experts, chips)),
            dma((experts, chips)),
            dma((experts,)),
            dma((experts,)),
        ],
        compiler_params=pltpu.CompilerParams(
            collective_id=2, has_side_effects=True, vmem_limit_bytes=67043328
        ),
        name="experts",
    )(buffer, gain, gate, up, down)


def eye_of(rows, columns):
    return lax.broadcasted_iota(jnp.int32, (rows, columns), 0) == lax.broadcasted_iota(jnp.int32, (rows, columns), 1)


def as_row(column, columns):
    rows = column.shape[0]
    return jnp.sum(jnp.where(eye_of(rows, columns), column, 0.0), axis=0, keepdims=True)


def routed(ids_ref, scale_ref, onehot, weigh, cuts, experts, exp):
    tokens = ids_ref.shape[1]
    relative = lax.broadcasted_iota(jnp.int32, (experts, tokens), 0)
    wanted = jnp.bitwise_xor(relative, exp)
    first, second = ids_ref[0:1, :] == wanted, ids_ref[1:2, :] == wanted
    member = (first | second).astype(jnp.float32)
    gates = jnp.where(first, scale_ref[0:1, :], 0.0) + jnp.where(second, scale_ref[1:2, :], 0.0)
    earlier = (
        lax.broadcasted_iota(jnp.int32, (tokens, tokens), 0) < lax.broadcasted_iota(jnp.int32, (tokens, tokens), 1)
    ).astype(jnp.bfloat16)
    place = jnp.dot(member.astype(jnp.bfloat16), earlier, preferred_element_type=jnp.float32)
    place = jnp.where(member > 0.5, place, -1.0).astype(jnp.int32)
    base = 0
    for r, count in enumerate(cuts):
        slots = base + lax.broadcasted_iota(jnp.int32, (count, tokens), 0)
        for k in range(experts):
            chosen = slots == place[k:k + 1, :]
            onehot[k, base:base + count, :] = chosen.astype(jnp.bfloat16)
            gate = jnp.where(chosen, gates[k:k + 1, :], 0.0)
            high = gate.astype(jnp.bfloat16)
            rows = pl.ds(k * count, count)
            weigh[r][0, rows, :] = high
            weigh[r][1, rows, :] = (gate - high.astype(jnp.float32)).astype(jnp.bfloat16)
        base += count


def square_experts_kernel(
    experts, cuts, residual, ids, scale, gain, gate_hbm, up_hbm, down_hbm, out,
    onehot, weigh_a, weigh_b, normal, buf_a, buf_b, rows_a, rows_b, wg, wu, wd, acc_g, acc_u, part_g, part_u, hidden_a, hidden_b,
    pair_a, pair_b, near_a, near_b, far_a, far_b, final_a, final_b, back_a, back_b, summed,
    sums, sums_in, inverse_out, inverse_in, inverse_a, inverse_b,
    w_sem, own_send, own_recv, near_send, near_recv, half_send, half_recv, pair_send, pair_recv,
    swap_send, swap_recv, one_send, one_recv, two_send, two_recv, ret_send, ret_recv,
    sum_send, sum_recv, inv_send, inv_recv,
):
    chips = 4
    ctx, exp = lax.axis_index("ctx"), lax.axis_index("exp")
    chip, core = ctx // 2, ctx % 2
    tokens, width = residual.shape
    features = gate_hbm.shape[2]
    inner = gate_hbm.shape[1]
    wing = width // 2
    cap = sum(cuts)
    weigh, buf, rows = (weigh_a, weigh_b), (buf_a, buf_b), (rows_a, rows_b)
    hidden, pair_in, near_in, far_in = (hidden_a, hidden_b), (pair_a, pair_b), (near_a, near_b), (far_a, far_b)
    final, back, inverse = (final_a, final_b), (back_a, back_b), (inverse_a, inverse_b)
    partner = (chip * 2 + 1 - core, exp)
    near = {j: (mixed(chip, j) * 2 + core, exp) for j in (1, 2)}
    peers = [(ctx, mixed(exp, k)) for k in range(1, experts)]
    plane = [(mixed(chip, j) * 2 + mixed(core, c), exp) for j in range(chips) for c in range(2)][1:]

    def f32(value):
        return value.astype(jnp.float32)

    def chunk(k):
        return pl.ds(k * width, width)

    loads, downs = [], []
    for k in range(experts):
        part = pl.ds(pl.multiple_of(mixed(exp, k) * width, width), width)
        loads.append((
            pltpu.make_async_copy(gate_hbm.at[0, :, part], wg.at[:, chunk(k)], w_sem.at[0, k]),
            pltpu.make_async_copy(up_hbm.at[0, :, part], wu.at[:, chunk(k)], w_sem.at[1, k]),
        ))
        downs.append(pltpu.make_async_copy(down_hbm.at[0, :, part], wd.at[k], w_sem.at[2, k]))
    for gate_load, up_load in loads:
        gate_load.start()
        up_load.start()
    for k in range(experts - 1, -1, -1):
        downs[k].start()

    def block(j, which):
        return which * chips + mixed(chip, j)

    def span(r, index):
        return pl.ds(pl.multiple_of(index * cuts[r], cuts[r]), cuts[r])

    def wings(k, way):
        return pl.ds(k * width + (way - 1) * wing, wing)

    mine = block(0, core)
    started = {"sums": [], 0: [], 1: [], "back": []}

    def begin(group, src, dst, send_sem, recv_sem, device):
        copy = remote(src, dst, send_sem, recv_sem, device)
        copy.start()
        started[group].append(copy)

    def arrive(view, recv_sem):
        remote(view, view, sum_send.at[0], recv_sem, partner).wait_recv()

    def settle(group):
        for copy in started[group]:
            copy.wait_send()
        started[group].clear()

    routed(ids, scale, onehot, weigh, cuts, experts, exp)
    greet(plane + peers)

    def prepare():
        x = f32(residual[...])
        normal[...] = (x * gain[exp]).astype(jnp.bfloat16)
        total = as_row(jnp.sum(x * x, axis=1, keepdims=True), tokens)
        sums[...] = jnp.broadcast_to(total, sums.shape)

    def route(r, k):
        base = sum(cuts[:r])
        picked = jnp.dot(
            onehot[k, base:base + cuts[r], :], normal[...], preferred_element_type=jnp.float32
        ).astype(jnp.bfloat16)
        if k == 0:
            rows[r][span(r, mine), chunk(0)] = picked
        else:
            buf[r][k] = picked
            begin(r, buf[r].at[k], rows[r].at[span(r, mine), chunk(k)], own_send.at[r, k], own_recv.at[r, k], peers[k - 1])

    def spread(r, k):
        here = rows[r].at[span(r, mine), chunk(k)]
        if k:
            arrive(here, own_recv.at[r, k])
        for j in (1, 2):
            begin(r, here, here, near_send.at[r, k, j], near_recv.at[r, k, j], near[j])
        begin(r, here, here, pair_send.at[r, k, 0], pair_recv.at[r, k, 0], partner)

    def forward(r, k):
        for j in (1, 2):
            place = span(r, block(j, core))
            here = rows[r].at[place, chunk(k)]
            arrive(here, near_recv.at[r, k, j])
            part = rows[r].at[place, wings(k, j)]
            begin(r, part, part, half_send.at[r, k, j], half_recv.at[r, k, j], near[3 - j])
            begin(r, here, here, pair_send.at[r, k, j], pair_recv.at[r, k, j], partner)

    def corner(r, k):
        place = span(r, block(3, core))
        for j in (1, 2):
            arrive(rows[r].at[place, wings(k, j)], half_recv.at[r, k, j])
        here = rows[r].at[place, chunk(k)]
        begin(r, here, here, pair_send.at[r, k, 3], pair_recv.at[r, k, 3], partner)

    def gathered(r, k):
        for j in range(chips):
            arrive(rows[r].at[span(r, block(j, 1 - core)), chunk(k)], pair_recv.at[r, k, j])
        if r == 0:
            loads[k][0].wait()
            loads[k][1].wait()

    def share_sums():
        for k in range(1, experts):
            begin("sums", sums, sums_in.at[k], sum_send.at[k], sum_recv.at[k], peers[k - 1])

    def share_inverse():
        total = sums[...]
        for k in range(1, experts):
            arrive(sums_in.at[k], sum_recv.at[k])
            total = total + sums_in[k]
        value = lax.rsqrt(total * (1.0 / features) + epsilon)[0:1, :]
        column = jnp.sum(jnp.where(onehot[0] > 0.5, value, 0.0), axis=1, keepdims=True)
        row = as_row(column, inverse_out.shape[1])
        inverse_out[...] = jnp.broadcast_to(row, inverse_out.shape)
        inverse_in[mine] = jnp.broadcast_to(row, inverse_out.shape)
        for n, device in enumerate(plane):
            begin("sums", inverse_out, inverse_in.at[mine], inv_send.at[n], inv_recv.at[mine], device)

    def take_inverse():
        for j in range(chips):
            for which in range(2):
                if j or which:
                    index = block(j, mixed(core, which))
                    arrive(inverse_in.at[index], inv_recv.at[index])
        for b in range(chips * 2):
            row = inverse_in[b][0:1, :]
            column = jnp.sum(jnp.where(eye_of(cap, row.shape[1]), row, 0.0), axis=1, keepdims=True)
            column = jnp.broadcast_to(column, (cap, 128))
            base = 0
            for r, count in enumerate(cuts):
                inverse[r][b * count:(b + 1) * count, :] = column[base:base + count, :]
                base += count

    def activate(r, at, g, u):
        by = inverse[r][:, 0:1]
        g = g * by
        u = u * by
        hidden[r][:, at] = (g / (1.0 + jnp.exp(-g)) * u).astype(jnp.bfloat16)

    tile = 512
    body = inner // tile * tile

    def up_tile(k):
        def one(at):
            g = times_transposed(rows_a[:, chunk(k)], wg[at, chunk(k)])
            u = times_transposed(rows_a[:, chunk(k)], wu[at, chunk(k)])
            if k:
                g = g + acc_g[:, at]
                u = u + acc_u[:, at]
            if k == experts - 1:
                activate(0, at, g, u)
            else:
                acc_g[:, at] = g
                acc_u[:, at] = u
        return one

    def expand_first(k):
        gathered(0, k)
        if k == experts - 1:
            take_inverse()
        if body:
            tiles(body, up_tile(k), tile)

    def expand_rest(k):
        if inner > body:
            up_tile(k)(pl.ds(body, inner - body))

    def whole_tile(at):
        rest = pl.ds(width, (experts - 1) * width)
        g = times_transposed(rows_b[:, rest], wg[at, rest]) + part_g[:, at]
        u = times_transposed(rows_b[:, rest], wu[at, rest]) + part_u[:, at]
        activate(1, at, g, u)

    def expand_part():
        gathered(1, 0)

        def one(at):
            part_g[:, at] = times_transposed(rows_b[:, chunk(0)], wg[at, chunk(0)])
            part_u[:, at] = times_transposed(rows_b[:, chunk(0)], wu[at, chunk(0)])

        tiles(inner, one, tile)

    def multiply(r, k):
        if r == 0:
            downs[k].wait()
        rows[r][:, chunk(k)] = jnp.dot(
            hidden[r][...], wd[k], preferred_element_type=jnp.float32
        ).astype(jnp.bfloat16)
        half = chips * cuts[r]
        there = pl.ds(pl.multiple_of((1 - core) * half, half), half)
        begin("back", rows[r].at[there, chunk(k)], pair_in[r].at[k], swap_send.at[r, k], swap_recv.at[r, k], partner)

    def paired(r, k, j, way):
        inside = pl.ds((way - 1) * wing, wing)
        return f32(rows[r][span(r, block(j, core)), wings(k, way)]) + f32(pair_in[r][k, span(r, mixed(chip, j)), inside])

    def merge(r, k):
        arrive(pair_in[r].at[k], swap_recv.at[r, k])
        for way in (1, 2):
            for slot, j in ((1, 3), (0, way)):
                here = (span(r, block(j, core)), wings(k, way))
                rows[r][here] = paired(r, k, j, way).astype(jnp.bfloat16)
                begin(
                    "back", rows[r].at[here], near_in[r].at[k, way - 1, slot],
                    one_send.at[r, k, way - 1, slot], one_recv.at[r, k, way - 1, slot], near[way],
                )

    def relay(r, k):
        for way in (1, 2):
            arrive(near_in[r].at[k, way - 1, 1], one_recv.at[r, k, way - 1, 1])
            j = 3 - way
            value = paired(r, k, j, way) + f32(near_in[r][k, way - 1, 1])
            here = (span(r, block(j, core)), wings(k, way))
            rows[r][here] = value.astype(jnp.bfloat16)
            begin(
                "back", rows[r].at[here], far_in[r].at[k, way - 1],
                two_send.at[r, k, way - 1], two_recv.at[r, k, way - 1], near[j],
            )

    def finish(r, k):
        for way in (1, 2):
            arrive(near_in[r].at[k, way - 1, 0], one_recv.at[r, k, way - 1, 0])
            arrive(far_in[r].at[k, way - 1], two_recv.at[r, k, way - 1])
            value = paired(r, k, 0, way) + f32(near_in[r][k, way - 1, 0]) + f32(far_in[r][k, way - 1])
            inside = pl.ds((way - 1) * wing, wing)
            if k == 0:
                back[r][0, :, inside] = value.astype(jnp.bfloat16)
            else:
                final[r][k, :, inside] = value.astype(jnp.bfloat16)
        if k:
            begin("back", final[r].at[k], back[r].at[k], ret_send.at[r, k], ret_recv.at[r, k], peers[k - 1])

    def combine(r):
        for k in range(1, experts):
            arrive(back[r].at[k], ret_recv.at[r, k])
        given = back[r][...].reshape(experts * cuts[r], width)
        value = f32(residual[...]) if r == 0 else summed[...]
        for which in range(2):
            value = value + lax.dot_general(
                weigh[r][which], given, (((0,), (0,)), ((), ())), preferred_element_type=jnp.float32
            )
        if r == 0:
            summed[...] = value
        else:
            out[...] = value.astype(jnp.bfloat16)

    prepare()
    share_sums()
    route(0, 0)
    spread(0, 0)
    for k in range(1, experts):
        route(0, k)
    route(1, 0)
    spread(1, 0)

    forward(0, 0)
    spread(0, 1)
    corner(0, 0)
    forward(1, 0)
    expand_first(0)
    forward(0, 1)
    spread(0, 2)
    corner(1, 0)
    expand_rest(0)
    for k in range(1, experts):
        route(1, k)
    expand_part()
    corner(0, 1)
    forward(0, 2)
    spread(0, 3)
    share_inverse()
    expand_first(1)
    corner(0, 2)
    forward(0, 3)
    spread(1, 1)
    expand_rest(1)
    expand_first(2)
    corner(0, 3)
    forward(1, 1)
    spread(1, 2)
    expand_rest(2)
    expand_first(3)
    corner(1, 1)
    forward(1, 2)
    spread(1, 3)
    expand_rest(3)
    settle(0)
    multiply(0, 3)
    corner(1, 2)
    forward(1, 3)
    multiply(0, 2)
    merge(0, 3)
    multiply(0, 1)
    merge(0, 2)
    multiply(0, 0)
    corner(1, 3)
    merge(0, 1)
    relay(0, 3)
    for k in range(1, experts):
        gathered(1, k)
    merge(0, 0)
    cuts_at = [pl.ds(at, min(tile, inner - at)) for at in range(0, inner, tile)]
    between = [
        ((relay, 2), (finish, 3)),
        ((relay, 1), (relay, 0), (finish, 2)),
        ((finish, 1), (finish, 0)),
    ]
    for n, at in enumerate(cuts_at):
        whole_tile(at)
        for action, k in between[n] if n < len(between) else ():
            action(0, k)
    for group in between[len(cuts_at):]:
        for action, k in group:
            action(0, k)
    settle(1)
    multiply(1, 3)
    multiply(1, 2)
    merge(1, 3)
    multiply(1, 1)
    merge(1, 2)
    multiply(1, 0)
    merge(1, 1)
    relay(1, 3)
    merge(1, 0)
    relay(1, 2)
    finish(1, 3)
    relay(1, 1)
    combine(0)
    finish(1, 2)
    relay(1, 0)
    finish(1, 1)
    finish(1, 0)
    combine(1)
    settle("back")
    settle("sums")


def run_square_experts(experts, cap, residual, ids, scale, gain, gate, up, down):
    tokens, width = residual.shape
    inner = gate.shape[1]
    chips = 4
    first = cap // 16 * 3 // 5 * 16
    cuts = (first, cap - first)
    bf16, f32 = jnp.bfloat16, jnp.float32
    dma = pltpu.SemaphoreType.DMA
    vmem = pl.BlockSpec(memory_space=pltpu.VMEM)
    hbm = pl.BlockSpec(memory_space=pl.ANY)

    def both(shape, dtype=bf16):
        return [pltpu.VMEM(shape(count), dtype) for count in cuts]

    return pl.pallas_call(
        functools.partial(square_experts_kernel, experts, cuts),
        out_shape=jax.ShapeDtypeStruct((tokens, width), bf16),
        in_specs=[vmem, vmem, vmem, vmem, hbm, hbm, hbm],
        out_specs=vmem,
        scratch_shapes=[
            pltpu.VMEM((experts, cap, tokens), bf16),
            *both(lambda n: (2, experts * n, tokens)),
            pltpu.VMEM((tokens, width), bf16),
            *both(lambda n: (experts, n, width)),
            *both(lambda n: (chips * 2 * n, experts * width)),
            pltpu.VMEM((inner, experts * width), bf16),
            pltpu.VMEM((inner, experts * width), bf16),
            pltpu.VMEM((experts, inner, width), bf16),
            pltpu.VMEM((chips * 2 * cuts[0], inner), f32),
            pltpu.VMEM((chips * 2 * cuts[0], inner), f32),
            pltpu.VMEM((chips * 2 * cuts[1], inner), f32),
            pltpu.VMEM((chips * 2 * cuts[1], inner), f32),
            *both(lambda n: (chips * 2 * n, inner)),
            *both(lambda n: (experts, chips * n, width)),
            *both(lambda n: (experts, 2, 2, n, width // 2)),
            *both(lambda n: (experts, 2, n, width // 2)),
            *both(lambda n: (experts, n, width)),
            *both(lambda n: (experts, n, width)),
            pltpu.VMEM((tokens, width), f32),
            pltpu.VMEM((8, tokens), f32),
            pltpu.VMEM((experts, 8, tokens), f32),
            pltpu.VMEM((8, 128), f32),
            pltpu.VMEM((chips * 2, 8, 128), f32),
            *both(lambda n: (chips * 2 * n, 128), f32),
            dma((3, experts)),
            dma((2, experts)),
            dma((2, experts)),
            dma((2, experts, 3)),
            dma((2, experts, 3)),
            dma((2, experts, 3)),
            dma((2, experts, 3)),
            dma((2, experts, 4)),
            dma((2, experts, 4)),
            dma((2, experts)),
            dma((2, experts)),
            dma((2, experts, 2, 2)),
            dma((2, experts, 2, 2)),
            dma((2, experts, 2)),
            dma((2, experts, 2)),
            dma((2, experts)),
            dma((2, experts)),
            dma((experts,)),
            dma((experts,)),
            dma((chips * 2 - 1,)),
            dma((chips * 2,)),
        ],
        compiler_params=pltpu.CompilerParams(
            collective_id=3, has_side_effects=True, vmem_limit_bytes=67043328
        ),
        name="square_experts",
    )(residual, ids, scale, gain, gate, up, down)


def attend(query_heads, key_rows, value_rows, query_offset):
    head_count, row_count, head_width = query_heads.shape
    key_count = key_rows.shape[0]
    key_split = key_rows.reshape(key_count, head_count, head_width)
    value_split = value_rows.reshape(key_count, head_count, head_width)
    scores = jnp.einsum(
        "hqd,khd->hqk", query_heads, key_split, preferred_element_type=jnp.float32
    ) * HEAD_DIM ** (-0.5)
    query_pos = query_offset + lax.broadcasted_iota(jnp.int32, (row_count, key_count), 0)
    key_pos = lax.broadcasted_iota(jnp.int32, (row_count, key_count), 1)
    visible = key_pos <= query_pos
    scores = jnp.where(visible[None], scores, masked_score)
    top = jnp.max(scores, axis=2)
    weights = jnp.where(visible[None], jnp.exp(scores - top[..., None]), 0.0)
    weighted = jnp.einsum(
        "hqk,khd->hqd",
        weights.astype(jnp.bfloat16),
        value_split,
        preferred_element_type=jnp.float32,
    )
    return weighted / jnp.sum(weights, axis=2)[..., None]


def local(
    hidden_in,
    query_vectors,
    key_vectors,
    value_vectors,
    out_weight,
    norm_gain,
    gate_proj,
    up_proj,
    down_proj,
    expert_ids,
    gate_scale,
):
    row_count, local_width = hidden_in.shape
    head_count = query_vectors.shape[1] // HEAD_DIM
    chips = lax.axis_size("ctx") // 2
    expert_count = lax.axis_size("exp")
    query_heads = query_vectors.reshape(row_count, head_count, HEAD_DIM).transpose(1, 0, 2)
    keys, values = gather_blocks(chips, key_vectors, value_vectors)
    attended = (
        attend(query_heads, keys, values, lax.axis_index("ctx") * row_count)
        .transpose(1, 0, 2)
        .reshape(row_count, head_count * HEAD_DIM)
        .astype(jnp.bfloat16)
    )
    capacity = min(row_count, 5 * row_count // (2 * expert_count))
    capacity = -(-capacity // 16) * 16
    if chips == 4 and expert_count == 4:
        residual = project(expert_count, attended, out_weight, hidden_in)
        return run_square_experts(
            expert_count,
            capacity,
            residual,
            expert_ids.T,
            gate_scale.T,
            norm_gain.reshape(expert_count, 1, local_width),
            gate_proj.transpose(0, 2, 1),
            up_proj.transpose(0, 2, 1),
            down_proj,
        )
    flat_ids = jnp.bitwise_xor(expert_ids.reshape(row_count * 2), lax.axis_index("exp"))
    onehot = (
        flat_ids[:, None] == lax.broadcasted_iota(jnp.int32, (row_count * 2, expert_count), 1)
    ).astype(jnp.int32)
    earlier = jnp.cumsum(onehot, axis=0) - onehot
    slot_index = jnp.sum(earlier * onehot, axis=1)
    target = flat_ids * capacity + slot_index
    placing = (
        target[None, :]
        == lax.broadcasted_iota(jnp.int32, (expert_count * capacity, row_count * 2), 0)
    ).astype(jnp.bfloat16)
    placing_tokens = jnp.sum(placing.reshape(expert_count * capacity, row_count, 2), axis=2)
    residual = project(expert_count, attended, out_weight, hidden_in)
    buffer = jnp.dot(placing_tokens, residual, preferred_element_type=jnp.float32).astype(
        jnp.bfloat16
    )
    returned = run_experts(
        chips,
        expert_count,
        buffer.reshape(expert_count, capacity, local_width),
        norm_gain.reshape(expert_count, 1, local_width),
        gate_proj.transpose(0, 2, 1),
        up_proj.transpose(0, 2, 1),
        down_proj,
    ).reshape(expert_count * capacity, local_width)
    gathered_back = lax.dot_general(
        placing, returned, (((0,), (0,)), ((), ())), preferred_element_type=jnp.float32
    )
    gathered_back = gathered_back.reshape(row_count, 2, local_width)
    combined = (
        residual.astype(jnp.float32)
        + gate_scale[:, 0:1] * gathered_back[:, 0]
        + gate_scale[:, 1:2] * gathered_back[:, 1]
    )
    return combined.astype(jnp.bfloat16)


def solution(mesh):
    placed = (
        P("ctx", "exp"),
        P("ctx", "exp"),
        P("ctx", "exp"),
        P("ctx", "exp"),
        P("exp", None),
        P(),
        P("exp", None, "ctx"),
        P("exp", None, "ctx"),
        P("exp", "ctx", None),
        P("ctx", None),
        P("ctx", None),
    )
    return jax.shard_map(
        local, mesh=mesh, in_specs=placed, out_specs=P("ctx", "exp"), check_vma=False
    )
```

```python
import functools

import jax
import jax.numpy as jnp
from jax import lax
from jax.experimental import pallas as pl
from jax.experimental.pallas import tpu as pltpu
from jax.sharding import PartitionSpec as P

HEAD_DIM = 128
MESH = pl.DeviceIdType.MESH

epsilon = 1e-05
masked_score = -1e30
PIECES = 4


def mixed(index, flip):
    result = index
    bit = 1
    while bit <= flip:
        if flip & bit:
            result = result + bit - 2 * bit * ((index // bit) % 2)
        bit *= 2
    return result


def remote(src, dst, send_sem, recv_sem, device):
    return pltpu.make_async_remote_copy(
        src_ref=src, dst_ref=dst, send_sem=send_sem, recv_sem=recv_sem,
        device_id=device, device_id_type=MESH,
    )


def greet(devices):
    barrier = pltpu.get_barrier_semaphore()
    for device in devices:
        pl.semaphore_signal(barrier, inc=1, device_id=device, device_id_type=MESH)
    pl.semaphore_wait(barrier, len(devices))


def gather_kernel(chips, k_ref, v_ref, ko_ref, vo_ref, local_sem, send_sem, pass_sem, recv_sem, half_send, half_recv):
    ctx, exp = lax.axis_index("ctx"), lax.axis_index("exp")
    chip, core = ctx // 2, ctx % 2
    rows = k_ref.shape[0]
    partner = (chip * 2 + 1 - core, exp)
    others = [(((chip + j) % chips) * 2 + core, exp) for j in range(1, chips)]
    pairs = ((k_ref, ko_ref), (v_ref, vo_ref))
    width = k_ref.shape[1]
    square = chips == 4
    near = (1, 2) if square else tuple(range(chips - 1, 0, -1))

    def device_of(j):
        return (mixed(chip, j) * 2 + core, exp) if square else others[j - 1]

    def source_of(j):
        return mixed(chip, j) if square else (chip + chips - j) % chips

    def half(ref, owner, which):
        part = pl.ds(pl.multiple_of(owner * rows, rows), rows)
        return ref.at[part, pl.ds(which * (width // 2), width // 2)]

    def block(ref, owner):
        return ref.at[pl.ds(pl.multiple_of(owner * rows, rows), rows), :]

    own = []
    for i, (src, dst) in enumerate(pairs):
        own.append(pltpu.make_async_copy(src, block(dst, ctx), local_sem.at[i]))
        own[-1].start()
    greet([partner] + others)
    sent = []
    for i, (src, dst) in enumerate(pairs):
        for j in near:
            sent.append(remote(src, block(dst, ctx), send_sem.at[i, j], recv_sem.at[i, ctx], device_of(j)))
            sent[-1].start()
        sent.append(remote(src, block(dst, ctx), send_sem.at[i, 0], recv_sem.at[i, ctx], partner))
        sent[-1].start()
    for i, (src, dst) in enumerate(pairs):
        for j in near:
            owner = source_of(j) * 2 + core
            here = block(dst, owner)
            passed = remote(here, here, pass_sem.at[i, j], recv_sem.at[i, owner], partner)
            passed.wait_recv()
            if square:
                piece = half(dst, owner, j - 1)
                sent.append(remote(piece, piece, half_send.at[i, j - 1], half_recv.at[i, j - 1], device_of(3 - j)))
                sent[-1].start()
            passed.start()
            sent.append(passed)
    for i, (src, dst) in enumerate(pairs):
        if square:
            owner = mixed(chip, 3) * 2 + core
            for h in range(2):
                piece = half(dst, owner, h)
                remote(piece, piece, half_send.at[i, h], half_recv.at[i, h], partner).wait_recv()
            here = block(dst, owner)
            sent.append(remote(here, here, pass_sem.at[i, 3], recv_sem.at[i, owner], partner))
            sent[-1].start()
    for i, (src, dst) in enumerate(pairs):
        for j in range(chips):
            owner = ((chip + chips - j) % chips) * 2 + 1 - core
            here = block(dst, owner)
            remote(here, here, pass_sem.at[i, 0], recv_sem.at[i, owner], partner).wait_recv()
    for copy in sent:
        copy.wait_send()
    for copy in own:
        copy.wait()


def gather_blocks(chips, keys, values):
    rows, width = keys.shape
    whole = jax.ShapeDtypeStruct((rows * chips * 2, width), keys.dtype)
    return pl.pallas_call(
        functools.partial(gather_kernel, chips),
        out_shape=(whole, whole),
        in_specs=[pl.BlockSpec(memory_space=pltpu.VMEM)] * 2,
        out_specs=[pl.BlockSpec(memory_space=pltpu.VMEM)] * 2,
        scratch_shapes=[
            pltpu.SemaphoreType.DMA((2,)),
            pltpu.SemaphoreType.DMA((2, chips)),
            pltpu.SemaphoreType.DMA((2, chips)),
            pltpu.SemaphoreType.DMA((2, chips * 2)),
            pltpu.SemaphoreType.DMA((2, 2)),
            pltpu.SemaphoreType.DMA((2, 2)),
        ],
        compiler_params=pltpu.CompilerParams(collective_id=0, has_side_effects=True),
        name="gather_blocks",
    )(keys, values)


def project_kernel(experts, att_ref, weight_ref, hidden_ref, out_ref, terms, landed, send_sem, recv_sem):
    ctx, exp = lax.axis_index("ctx"), lax.axis_index("exp")
    width = hidden_ref.shape[1]
    levels = experts.bit_length() - 1
    depth = hidden_ref.shape[0] // PIECES
    peers = [(ctx, mixed(exp, 1 << b)) for b in range(levels)]
    greet(peers)
    sent = []

    def slot(level, k):
        return sum(experts >> (b + 1) for b in range(level)) + k // (2 << level)

    def send(level, k, piece):
        to = slot(level, k - (1 << level))
        here = pl.ds(piece * depth, depth)
        sent.append(remote(
            terms.at[k, here], landed.at[to, here], send_sem.at[to, piece], recv_sem.at[to, piece], peers[level]
        ))
        sent[-1].start()

    order = [k for k in range(experts - 1, -1, -1) if k % 2] + [k for k in range(experts - 1, -1, -1) if not k % 2]
    for k in order:
        columns = pl.ds(pl.multiple_of(mixed(exp, k) * width, width), width)
        terms[k] = jnp.dot(
            att_ref[...], weight_ref[:, columns], preferred_element_type=jnp.float32
        ).astype(jnp.bfloat16)
        if k % 2:
            for piece in range(PIECES):
                send(0, k, piece)
    for level in range(levels):
        for k in range(experts - (2 << level), -1, -(2 << level)):
            at = slot(level, k)
            for piece in range(PIECES):
                here = pl.ds(piece * depth, depth)
                view = landed.at[at, here]
                remote(view, view, send_sem.at[at, piece], recv_sem.at[at, piece], peers[level]).wait_recv()
                total = terms[k, here, :].astype(jnp.float32) + landed[at, here, :].astype(jnp.float32)
                if level + 1 < levels:
                    terms[k, here, :] = total.astype(jnp.bfloat16)
                    if k & (2 << level):
                        send(level + 1, k, piece)
                else:
                    out_ref[here, :] = (hidden_ref[here, :].astype(jnp.float32) + total).astype(jnp.bfloat16)
    for copy in sent:
        copy.wait_send()


def project(experts, attended, weight, hidden):
    rows, width = hidden.shape
    return pl.pallas_call(
        functools.partial(project_kernel, experts),
        out_shape=jax.ShapeDtypeStruct((rows, width), jnp.bfloat16),
        in_specs=[pl.BlockSpec(memory_space=pltpu.VMEM)] * 3,
        out_specs=pl.BlockSpec(memory_space=pltpu.VMEM),
        scratch_shapes=[
            pltpu.VMEM((experts, rows, width), jnp.bfloat16),
            pltpu.VMEM((experts - 1, rows, width), jnp.bfloat16),
            pltpu.SemaphoreType.DMA((experts - 1, PIECES)),
            pltpu.SemaphoreType.DMA((experts - 1, PIECES)),
        ],
        compiler_params=pltpu.CompilerParams(
            collective_id=1, has_side_effects=True, vmem_limit_bytes=32 * 1024 * 1024
        ),
        name="project_reduce",
    )(attended, weight, hidden)


def tiles(width, body, size=256):
    full = width // size
    if full:
        @pl.loop(0, full)
        def _(t):
            body(pl.ds(pl.multiple_of(t * size, size), size))
    if width % size:
        body(pl.ds(full * size, width % size))


def times_transposed(left, right):
    return lax.dot_general(
        left, right, (((1,), (1,)), ((), ())), preferred_element_type=jnp.float32
    )


def experts_kernel(
    chips, experts, buf, gain, gate_hbm, up_hbm, down_hbm, out,
    rows_all, wg, wu, wd, acc_g, acc_u, scaled, hidden, squares, pair_in, chip_in, final,
    w_sem, local_sem, a2a_send, ag_send, pass_send, ag_recv,
    pair_send, pair_recv, rs_send, rs_recv, ret_send, ret_recv,
):
    ctx, exp = lax.axis_index("ctx"), lax.axis_index("exp")
    chip, core = ctx // 2, ctx % 2
    cap, width = buf.shape[1:]
    total_rows = chips * 2 * cap
    features = gate_hbm.shape[2]
    inner = gate_hbm.shape[1]
    partner = (chip * 2 + 1 - core, exp)
    others = [(((chip + j) % chips) * 2 + core, exp) for j in range(1, chips)]
    peers = [(ctx, mixed(exp, k)) for k in range(1, experts)]

    loads = []
    for k in range(experts):
        part = pl.ds(pl.multiple_of(mixed(exp, k) * width, width), width)
        loads.append((
            pltpu.make_async_copy(gate_hbm.at[0, :, part], wg.at[k], w_sem.at[0, k]),
            pltpu.make_async_copy(up_hbm.at[0, :, part], wu.at[k], w_sem.at[1, k]),
        ))
    downs = []
    for k in range(experts):
        part = pl.ds(pl.multiple_of(mixed(exp, k) * width, width), width)
        downs.append(pltpu.make_async_copy(down_hbm.at[0, :, part], wd.at[k], w_sem.at[2, k]))

    def span(index):
        return pl.ds(pl.multiple_of(index * cap, cap), cap)

    mine = core * chips + chip

    own = pltpu.make_async_copy(buf.at[0], rows_all.at[0, span(mine), :], local_sem.at[0])
    own.start()
    for gate_load, up_load in loads:
        gate_load.start()
        up_load.start()
    for k in range(experts - 1, -1, -1):
        downs[k].start()
    greet([partner] + others + peers)

    sent = []
    for k in range(1, experts):
        copy = remote(buf.at[k], rows_all.at[k, span(mine), :], a2a_send.at[k], ag_recv.at[k, mine], peers[k - 1])
        copy.start()
        sent.append(copy)

    def spread(k):
        here = rows_all.at[k, span(mine), :]
        if k == 0:
            own.wait()
        else:
            remote(here, here, a2a_send.at[k], ag_recv.at[k, mine], partner).wait_recv()
        for j in range(chips - 1, 0, -1):
            copy = remote(here, here, ag_send.at[k, j], ag_recv.at[k, mine], others[j - 1])
            copy.start()
            sent.append(copy)
        copy = remote(here, here, ag_send.at[k, 0], ag_recv.at[k, mine], partner)
        copy.start()
        sent.append(copy)

    def collect(k):
        for j in range(1, chips):
            owner = core * chips + (chip + chips - j) % chips
            here = rows_all.at[k, span(owner), :]
            copy = remote(here, here, pass_send.at[k, j], ag_recv.at[k, owner], partner)
            copy.wait_recv()
            copy.start()
            sent.append(copy)
        for j in range(chips):
            owner = (1 - core) * chips + (chip + chips - j) % chips
            here = rows_all.at[k, span(owner), :]
            remote(here, here, pass_send.at[k, 0], ag_recv.at[k, owner], partner).wait_recv()

    spread(0)
    spread(1)
    for k in range(experts):
        collect(k)
        if k + 2 < experts:
            spread(k + 2)
        gain_row = gain[mixed(exp, k)]

        @pl.loop(0, chips * 2)
        def _(b, k=k, gain_row=gain_row):
            x = rows_all[k, span(b), :].astype(jnp.float32)
            square = jnp.broadcast_to(jnp.sum(x * x, axis=1, keepdims=True), (cap, 128))
            squares[span(b), :] = square if k == 0 else squares[span(b), :] + square
            scaled[span(b), :] = (x * gain_row).astype(jnp.bfloat16)

        loads[k][0].wait()
        loads[k][1].wait()
        last = k == experts - 1
        if last:
            squares[...] = lax.rsqrt(squares[...] * (1.0 / features) + epsilon)

        def up_tile(cols, k=k, last=last):
            g = times_transposed(scaled[...], wg[k, cols, :])
            u = times_transposed(scaled[...], wu[k, cols, :])
            if k:
                g = g + acc_g[:, cols]
                u = u + acc_u[:, cols]
            if last:
                inverse = squares[:, 0:1]
                g = g * inverse
                u = u * inverse
                hidden[:, cols] = (g / (1.0 + jnp.exp(-g)) * u).astype(jnp.bfloat16)
            else:
                acc_g[:, cols] = g
                acc_u[:, cols] = u

        tiles(inner, up_tile)

    for copy in sent:
        copy.wait_send()
    sent = []
    half = chips * cap

    def half_of(which):
        return pl.ds(pl.multiple_of(which * half, half), half)

    def multiply(k):
        downs[k].wait()

        def down_tile(cols):
            rows_all[k, :, cols] = jnp.dot(
                hidden[...], wd[k, :, cols], preferred_element_type=jnp.float32
            ).astype(jnp.bfloat16)

        tiles(width, down_tile)
        copy = remote(rows_all.at[k, half_of(1 - core), :], pair_in.at[k], pair_send.at[k], pair_recv.at[k], partner)
        copy.start()
        sent.append(copy)

    def merge(k):
        remote(pair_in.at[k], pair_in.at[k], pair_send.at[k], pair_recv.at[k], partner).wait_recv()
        for j in range(chips - 1, -1, -1):
            to = (chip + j) % chips
            place = span(core * chips + to)
            rows_all[k, place, :] = (
                rows_all[k, place, :].astype(jnp.float32) + pair_in[k, span(to), :].astype(jnp.float32)
            ).astype(jnp.bfloat16)
            if j:
                copy = remote(rows_all.at[k, place, :], chip_in.at[k, j - 1], rs_send.at[k, j], rs_recv.at[k, j], others[j - 1])
                copy.start()
                sent.append(copy)

    def finish(k):
        value = rows_all[k, span(mine), :].astype(jnp.float32)
        for j in range(1, chips):
            here = chip_in.at[k, j - 1]
            remote(here, here, rs_send.at[k, j], rs_recv.at[k, j], partner).wait_recv()
            value = value + chip_in[k, j - 1].astype(jnp.float32)
        if k == 0:
            out[0] = value.astype(jnp.bfloat16)
        else:
            final[k] = value.astype(jnp.bfloat16)
            copy = remote(final.at[k], out.at[k], ret_send.at[k], ret_recv.at[k], peers[k - 1])
            copy.start()
            sent.append(copy)

    order = list(range(experts - 1, -1, -1))
    for step in range(experts + 2):
        if step < experts:
            multiply(order[step])
        if 1 <= step <= experts:
            merge(order[step - 1])
        if step >= 2:
            finish(order[step - 2])
    for k in range(1, experts):
        remote(out.at[k], out.at[k], ret_send.at[k], ret_recv.at[k], peers[k - 1]).wait_recv()
    for copy in sent:
        copy.wait_send()


def run_experts(chips, experts, buffer, gain, gate, up, down):
    _, cap, width = buffer.shape
    inner = gate.shape[1]
    rows = chips * 2 * cap
    bf16, f32 = jnp.bfloat16, jnp.float32
    dma = pltpu.SemaphoreType.DMA
    vmem = pl.BlockSpec(memory_space=pltpu.VMEM)
    hbm = pl.BlockSpec(memory_space=pl.ANY)
    return pl.pallas_call(
        functools.partial(experts_kernel, chips, experts),
        out_shape=jax.ShapeDtypeStruct((experts, cap, width), bf16),
        in_specs=[vmem, vmem, hbm, hbm, hbm],
        out_specs=vmem,
        scratch_shapes=[
            pltpu.VMEM((experts, rows, width), bf16),
            pltpu.VMEM((experts, inner, width), bf16),
            pltpu.VMEM((experts, inner, width), bf16),
            pltpu.VMEM((experts, inner, width), bf16),
            pltpu.VMEM((rows, inner), f32),
            pltpu.VMEM((rows, inner), f32),
            pltpu.VMEM((rows, width), bf16),
            pltpu.VMEM((rows, inner), bf16),
            pltpu.VMEM((rows, 128), f32),
            pltpu.VMEM((experts, chips * cap, width), bf16),
            pltpu.VMEM((experts, chips - 1, cap, width), bf16),
            pltpu.VMEM((experts, cap, width), bf16),
            dma((3, experts)),
            dma((1,)),
            dma((experts,)),
            dma((experts, chips)),
            dma((experts, chips)),
            dma((experts, chips * 2)),
            dma((experts,)),
            dma((experts,)),
            dma((experts, chips)),
            dma((experts, chips)),
            dma((experts,)),
            dma((experts,)),
        ],
        compiler_params=pltpu.CompilerParams(
            collective_id=2, has_side_effects=True, vmem_limit_bytes=67043328
        ),
        name="experts",
    )(buffer, gain, gate, up, down)


def eye_of(rows, columns):
    return lax.broadcasted_iota(jnp.int32, (rows, columns), 0) == lax.broadcasted_iota(jnp.int32, (rows, columns), 1)


def as_row(column, columns):
    rows = column.shape[0]
    return jnp.sum(jnp.where(eye_of(rows, columns), column, 0.0), axis=0, keepdims=True)


def routed(ids_ref, scale_ref, onehot, weigh, cuts, experts, exp):
    tokens = ids_ref.shape[1]
    relative = lax.broadcasted_iota(jnp.int32, (experts, tokens), 0)
    wanted = jnp.bitwise_xor(relative, exp)
    first, second = ids_ref[0:1, :] == wanted, ids_ref[1:2, :] == wanted
    member = (first | second).astype(jnp.float32)
    gates = jnp.where(first, scale_ref[0:1, :], 0.0) + jnp.where(second, scale_ref[1:2, :], 0.0)
    earlier = (
        lax.broadcasted_iota(jnp.int32, (tokens, tokens), 0) < lax.broadcasted_iota(jnp.int32, (tokens, tokens), 1)
    ).astype(jnp.bfloat16)
    place = jnp.dot(member.astype(jnp.bfloat16), earlier, preferred_element_type=jnp.float32)
    place = jnp.where(member > 0.5, place, -1.0).astype(jnp.int32)
    base = 0
    for r, count in enumerate(cuts):
        slots = base + lax.broadcasted_iota(jnp.int32, (count, tokens), 0)
        for k in range(experts):
            chosen = slots == place[k:k + 1, :]
            onehot[k, base:base + count, :] = chosen.astype(jnp.bfloat16)
            gate = jnp.where(chosen, gates[k:k + 1, :], 0.0)
            high = gate.astype(jnp.bfloat16)
            rows = pl.ds(k * count, count)
            weigh[r][0, rows, :] = high
            weigh[r][1, rows, :] = (gate - high.astype(jnp.float32)).astype(jnp.bfloat16)
        base += count


def square_experts_kernel(
    experts, cuts, residual, ids, scale, gain, gate_hbm, up_hbm, down_hbm, out,
    onehot, weigh_a, weigh_b, normal, buf_a, buf_b, rows_a, rows_b, wg, wu, wd, acc_g, acc_u, part_g, part_u, hidden_a, hidden_b,
    pair_a, pair_b, near_a, near_b, far_a, far_b, final_a, final_b, back_a, back_b, summed,
    sums, sums_in, inverse_out, inverse_in, inverse_a, inverse_b,
    w_sem, own_send, own_recv, near_send, near_recv, half_send, half_recv, pair_send, pair_recv,
    swap_send, swap_recv, one_send, one_recv, two_send, two_recv, ret_send, ret_recv,
    sum_send, sum_recv, inv_send, inv_recv,
):
    chips = 4
    ctx, exp = lax.axis_index("ctx"), lax.axis_index("exp")
    chip, core = ctx // 2, ctx % 2
    tokens, width = residual.shape
    features = gate_hbm.shape[2]
    inner = gate_hbm.shape[1]
    wing = width // 2
    cap = sum(cuts)
    weigh, buf, rows = (weigh_a, weigh_b), (buf_a, buf_b), (rows_a, rows_b)
    hidden, pair_in, near_in, far_in = (hidden_a, hidden_b), (pair_a, pair_b), (near_a, near_b), (far_a, far_b)
    final, back, inverse = (final_a, final_b), (back_a, back_b), (inverse_a, inverse_b)
    partner = (chip * 2 + 1 - core, exp)
    near = {j: (mixed(chip, j) * 2 + core, exp) for j in (1, 2)}
    peers = [(ctx, mixed(exp, k)) for k in range(1, experts)]
    plane = [(mixed(chip, j) * 2 + mixed(core, c), exp) for j in range(chips) for c in range(2)][1:]

    def f32(value):
        return value.astype(jnp.float32)

    def chunk(k):
        return pl.ds(k * width, width)

    loads, downs = [], []
    for k in range(experts):
        part = pl.ds(pl.multiple_of(mixed(exp, k) * width, width), width)
        loads.append((
            pltpu.make_async_copy(gate_hbm.at[0, :, part], wg.at[:, chunk(k)], w_sem.at[0, k]),
            pltpu.make_async_copy(up_hbm.at[0, :, part], wu.at[:, chunk(k)], w_sem.at[1, k]),
        ))
        downs.append(pltpu.make_async_copy(down_hbm.at[0, :, part], wd.at[k], w_sem.at[2, k]))
    for gate_load, up_load in loads:
        gate_load.start()
        up_load.start()
    for k in range(experts - 1, -1, -1):
        downs[k].start()

    def block(j, which):
        return which * chips + mixed(chip, j)

    def span(r, index):
        return pl.ds(pl.multiple_of(index * cuts[r], cuts[r]), cuts[r])

    def wings(k, way):
        return pl.ds(k * width + (way - 1) * wing, wing)

    mine = block(0, core)
    started = {"sums": [], 0: [], 1: [], "back": []}

    def begin(group, src, dst, send_sem, recv_sem, device):
        copy = remote(src, dst, send_sem, recv_sem, device)
        copy.start()
        started[group].append(copy)

    def arrive(view, recv_sem):
        remote(view, view, sum_send.at[0], recv_sem, partner).wait_recv()

    def settle(group):
        for copy in started[group]:
            copy.wait_send()
        started[group].clear()

    routed(ids, scale, onehot, weigh, cuts, experts, exp)
    greet(plane + peers)

    def prepare():
        x = f32(residual[...])
        normal[...] = (x * gain[exp]).astype(jnp.bfloat16)
        total = as_row(jnp.sum(x * x, axis=1, keepdims=True), tokens)
        sums[...] = jnp.broadcast_to(total, sums.shape)

    def route(r, k):
        base = sum(cuts[:r])
        picked = jnp.dot(
            onehot[k, base:base + cuts[r], :], normal[...], preferred_element_type=jnp.float32
        ).astype(jnp.bfloat16)
        if k == 0:
            rows[r][span(r, mine), chunk(0)] = picked
        else:
            buf[r][k] = picked
            begin(r, buf[r].at[k], rows[r].at[span(r, mine), chunk(k)], own_send.at[r, k], own_recv.at[r, k], peers[k - 1])

    def spread(r, k):
        here = rows[r].at[span(r, mine), chunk(k)]
        if k:
            arrive(here, own_recv.at[r, k])
        for j in (1, 2):
            begin(r, here, here, near_send.at[r, k, j], near_recv.at[r, k, j], near[j])
        begin(r, here, here, pair_send.at[r, k, 0], pair_recv.at[r, k, 0], partner)

    def forward(r, k):
        for j in (1, 2):
            place = span(r, block(j, core))
            here = rows[r].at[place, chunk(k)]
            arrive(here, near_recv.at[r, k, j])
            part = rows[r].at[place, wings(k, j)]
            begin(r, part, part, half_send.at[r, k, j], half_recv.at[r, k, j], near[3 - j])
            begin(r, here, here, pair_send.at[r, k, j], pair_recv.at[r, k, j], partner)

    def corner(r, k):
        place = span(r, block(3, core))
        for j in (1, 2):
            arrive(rows[r].at[place, wings(k, j)], half_recv.at[r, k, j])
        here = rows[r].at[place, chunk(k)]
        begin(r, here, here, pair_send.at[r, k, 3], pair_recv.at[r, k, 3], partner)

    def gathered(r, k):
        for j in range(chips):
            arrive(rows[r].at[span(r, block(j, 1 - core)), chunk(k)], pair_recv.at[r, k, j])
        if r == 0:
            loads[k][0].wait()
            loads[k][1].wait()

    def share_sums():
        for k in range(1, experts):
            begin("sums", sums, sums_in.at[k], sum_send.at[k], sum_recv.at[k], peers[k - 1])

    def share_inverse():
        total = sums[...]
        for k in range(1, experts):
            arrive(sums_in.at[k], sum_recv.at[k])
            total = total + sums_in[k]
        value = lax.rsqrt(total * (1.0 / features) + epsilon)[0:1, :]
        column = jnp.sum(jnp.where(onehot[0] > 0.5, value, 0.0), axis=1, keepdims=True)
        row = as_row(column, inverse_out.shape[1])
        inverse_out[...] = jnp.broadcast_to(row, inverse_out.shape)
        inverse_in[mine] = jnp.broadcast_to(row, inverse_out.shape)
        for n, device in enumerate(plane):
            begin("sums", inverse_out, inverse_in.at[mine], inv_send.at[n], inv_recv.at[mine], device)

    def take_inverse():
        for j in range(chips):
            for which in range(2):
                if j or which:
                    index = block(j, mixed(core, which))
                    arrive(inverse_in.at[index], inv_recv.at[index])
        for b in range(chips * 2):
            row = inverse_in[b][0:1, :]
            column = jnp.sum(jnp.where(eye_of(cap, row.shape[1]), row, 0.0), axis=1, keepdims=True)
            column = jnp.broadcast_to(column, (cap, 128))
            base = 0
            for r, count in enumerate(cuts):
                inverse[r][b * count:(b + 1) * count, :] = column[base:base + count, :]
                base += count

    def activate(r, at, g, u):
        by = inverse[r][:, 0:1]
        g = g * by
        u = u * by
        hidden[r][:, at] = (g / (1.0 + jnp.exp(-g)) * u).astype(jnp.bfloat16)

    tile = 512
    body = inner // tile * tile

    def up_tile(k):
        def one(at):
            g = times_transposed(rows_a[:, chunk(k)], wg[at, chunk(k)])
            u = times_transposed(rows_a[:, chunk(k)], wu[at, chunk(k)])
            if k:
                g = g + acc_g[:, at]
                u = u + acc_u[:, at]
            if k == experts - 1:
                activate(0, at, g, u)
            else:
                acc_g[:, at] = g
                acc_u[:, at] = u
        return one

    def expand_first(k):
        gathered(0, k)
        if k == experts - 1:
            take_inverse()
        if body:
            tiles(body, up_tile(k), tile)

    def expand_rest(k):
        if inner > body:
            up_tile(k)(pl.ds(body, inner - body))

    def whole_tile(at):
        rest = pl.ds(width, (experts - 1) * width)
        g = times_transposed(rows_b[:, rest], wg[at, rest]) + part_g[:, at]
        u = times_transposed(rows_b[:, rest], wu[at, rest]) + part_u[:, at]
        activate(1, at, g, u)

    def expand_part():
        gathered(1, 0)

        def one(at):
            part_g[:, at] = times_transposed(rows_b[:, chunk(0)], wg[at, chunk(0)])
            part_u[:, at] = times_transposed(rows_b[:, chunk(0)], wu[at, chunk(0)])

        tiles(inner, one, tile)

    def multiply(r, k):
        if r == 0:
            downs[k].wait()
        rows[r][:, chunk(k)] = jnp.dot(
            hidden[r][...], wd[k], preferred_element_type=jnp.float32
        ).astype(jnp.bfloat16)
        half = chips * cuts[r]
        there = pl.ds(pl.multiple_of((1 - core) * half, half), half)
        begin("back", rows[r].at[there, chunk(k)], pair_in[r].at[k], swap_send.at[r, k], swap_recv.at[r, k], partner)

    def paired(r, k, j, way):
        inside = pl.ds((way - 1) * wing, wing)
        return f32(rows[r][span(r, block(j, core)), wings(k, way)]) + f32(pair_in[r][k, span(r, mixed(chip, j)), inside])

    def merge(r, k):
        arrive(pair_in[r].at[k], swap_recv.at[r, k])
        for way in (1, 2):
            for slot, j in ((1, 3), (0, way)):
                here = (span(r, block(j, core)), wings(k, way))
                rows[r][here] = paired(r, k, j, way).astype(jnp.bfloat16)
                begin(
                    "back", rows[r].at[here], near_in[r].at[k, way - 1, slot],
                    one_send.at[r, k, way - 1, slot], one_recv.at[r, k, way - 1, slot], near[way],
                )

    def relay(r, k):
        for way in (1, 2):
            arrive(near_in[r].at[k, way - 1, 1], one_recv.at[r, k, way - 1, 1])
            j = 3 - way
            value = paired(r, k, j, way) + f32(near_in[r][k, way - 1, 1])
            here = (span(r, block(j, core)), wings(k, way))
            rows[r][here] = value.astype(jnp.bfloat16)
            begin(
                "back", rows[r].at[here], far_in[r].at[k, way - 1],
                two_send.at[r, k, way - 1], two_recv.at[r, k, way - 1], near[j],
            )

    def finish(r, k):
        for way in (1, 2):
            arrive(near_in[r].at[k, way - 1, 0], one_recv.at[r, k, way - 1, 0])
            arrive(far_in[r].at[k, way - 1], two_recv.at[r, k, way - 1])
            value = paired(r, k, 0, way) + f32(near_in[r][k, way - 1, 0]) + f32(far_in[r][k, way - 1])
            inside = pl.ds((way - 1) * wing, wing)
            if k == 0:
                back[r][0, :, inside] = value.astype(jnp.bfloat16)
            else:
                final[r][k, :, inside] = value.astype(jnp.bfloat16)
        if k:
            begin("back", final[r].at[k], back[r].at[k], ret_send.at[r, k], ret_recv.at[r, k], peers[k - 1])

    def combine(r):
        for k in range(1, experts):
            arrive(back[r].at[k], ret_recv.at[r, k])
        given = back[r][...].reshape(experts * cuts[r], width)
        value = f32(residual[...]) if r == 0 else summed[...]
        for which in range(2):
            value = value + lax.dot_general(
                weigh[r][which], given, (((0,), (0,)), ((), ())), preferred_element_type=jnp.float32
            )
        if r == 0:
            summed[...] = value
        else:
            out[...] = value.astype(jnp.bfloat16)

    prepare()
    share_sums()
    route(0, 0)
    spread(0, 0)
    for k in range(1, experts):
        route(0, k)
    route(1, 0)
    spread(1, 0)

    forward(0, 0)
    spread(0, 1)
    corner(0, 0)
    forward(1, 0)
    expand_first(0)
    forward(0, 1)
    spread(0, 2)
    corner(1, 0)
    expand_rest(0)
    for k in range(1, experts):
        route(1, k)
    expand_part()
    corner(0, 1)
    forward(0, 2)
    spread(0, 3)
    share_inverse()
    expand_first(1)
    corner(0, 2)
    forward(0, 3)
    spread(1, 1)
    expand_rest(1)
    expand_first(2)
    corner(0, 3)
    forward(1, 1)
    spread(1, 2)
    expand_rest(2)
    expand_first(3)
    corner(1, 1)
    forward(1, 2)
    spread(1, 3)
    expand_rest(3)
    settle(0)
    multiply(0, 3)
    corner(1, 2)
    forward(1, 3)
    multiply(0, 2)
    merge(0, 3)
    multiply(0, 1)
    merge(0, 2)
    multiply(0, 0)
    corner(1, 3)
    merge(0, 1)
    relay(0, 3)
    for k in range(1, experts):
        gathered(1, k)
    merge(0, 0)
    cuts_at = [pl.ds(at, min(tile, inner - at)) for at in range(0, inner, tile)]
    between = [
        ((relay, 2), (finish, 3)),
        ((relay, 1), (relay, 0), (finish, 2)),
        ((finish, 1), (finish, 0)),
    ]
    for n, at in enumerate(cuts_at):
        whole_tile(at)
        for action, k in between[n] if n < len(between) else ():
            action(0, k)
    for group in between[len(cuts_at):]:
        for action, k in group:
            action(0, k)
    settle(1)
    multiply(1, 3)
    multiply(1, 2)
    merge(1, 3)
    multiply(1, 1)
    merge(1, 2)
    multiply(1, 0)
    merge(1, 1)
    relay(1, 3)
    merge(1, 0)
    relay(1, 2)
    finish(1, 3)
    relay(1, 1)
    combine(0)
    finish(1, 2)
    relay(1, 0)
    finish(1, 1)
    finish(1, 0)
    combine(1)
    settle("back")
    settle("sums")


def run_square_experts(experts, cap, residual, ids, scale, gain, gate, up, down):
    tokens, width = residual.shape
    inner = gate.shape[1]
    chips = 4
    first = cap // 16 * 3 // 5 * 16
    cuts = (first, cap - first)
    bf16, f32 = jnp.bfloat16, jnp.float32
    dma = pltpu.SemaphoreType.DMA
    vmem = pl.BlockSpec(memory_space=pltpu.VMEM)
    hbm = pl.BlockSpec(memory_space=pl.ANY)

    def both(shape, dtype=bf16):
        return [pltpu.VMEM(shape(count), dtype) for count in cuts]

    return pl.pallas_call(
        functools.partial(square_experts_kernel, experts, cuts),
        out_shape=jax.ShapeDtypeStruct((tokens, width), bf16),
        in_specs=[vmem, vmem, vmem, vmem, hbm, hbm, hbm],
        out_specs=vmem,
        scratch_shapes=[
            pltpu.VMEM((experts, cap, tokens), bf16),
            *both(lambda n: (2, experts * n, tokens)),
            pltpu.VMEM((tokens, width), bf16),
            *both(lambda n: (experts, n, width)),
            *both(lambda n: (chips * 2 * n, experts * width)),
            pltpu.VMEM((inner, experts * width), bf16),
            pltpu.VMEM((inner, experts * width), bf16),
            pltpu.VMEM((experts, inner, width), bf16),
            pltpu.VMEM((chips * 2 * cuts[0], inner), f32),
            pltpu.VMEM((chips * 2 * cuts[0], inner), f32),
            pltpu.VMEM((chips * 2 * cuts[1], inner), f32),
            pltpu.VMEM((chips * 2 * cuts[1], inner), f32),
            *both(lambda n: (chips * 2 * n, inner)),
            *both(lambda n: (experts, chips * n, width)),
            *both(lambda n: (experts, 2, 2, n, width // 2)),
            *both(lambda n: (experts, 2, n, width // 2)),
            *both(lambda n: (experts, n, width)),
            *both(lambda n: (experts, n, width)),
            pltpu.VMEM((tokens, width), f32),
            pltpu.VMEM((8, tokens), f32),
            pltpu.VMEM((experts, 8, tokens), f32),
            pltpu.VMEM((8, 128), f32),
            pltpu.VMEM((chips * 2, 8, 128), f32),
            *both(lambda n: (chips * 2 * n, 128), f32),
            dma((3, experts)),
            dma((2, experts)),
            dma((2, experts)),
            dma((2, experts, 3)),
            dma((2, experts, 3)),
            dma((2, experts, 3)),
            dma((2, experts, 3)),
            dma((2, experts, 4)),
            dma((2, experts, 4)),
            dma((2, experts)),
            dma((2, experts)),
            dma((2, experts, 2, 2)),
            dma((2, experts, 2, 2)),
            dma((2, experts, 2)),
            dma((2, experts, 2)),
            dma((2, experts)),
            dma((2, experts)),
            dma((experts,)),
            dma((experts,)),
            dma((chips * 2 - 1,)),
            dma((chips * 2,)),
        ],
        compiler_params=pltpu.CompilerParams(
            collective_id=3, has_side_effects=True, vmem_limit_bytes=67043328
        ),
        name="square_experts",
    )(residual, ids, scale, gain, gate, up, down)


def attend_kernel(
    experts, query_hbm, key_hbm, value_hbm, hidden_hbm, weight_hbm, out,
    query, hidden, keys, values, share, own_weight, walls, att,
    load_sem, near_send, near_recv, half_send, half_recv, pair_send, pair_recv,
    share_send, share_recv, att_send, att_recv,
):
    chips = 4
    ctx, exp = lax.axis_index("ctx"), lax.axis_index("exp")
    chip, core = ctx // 2, ctx % 2
    tokens, depth = query.shape
    width = hidden.shape[1]
    heads = depth // HEAD_DIM
    strip = share.shape[1]
    partner = (chip * 2 + 1 - core, exp)
    near = {j: (mixed(chip, j) * 2 + core, exp) for j in (1, 2)}
    peers = [(ctx, mixed(exp, k)) for k in range(1, experts)]
    arrays = [keys, values] + [walls.at[k] for k in range(experts - 1)]

    def columns(k):
        return pl.ds(pl.multiple_of(mixed(exp, k) * width, width), width)

    mine = pl.ds(pl.multiple_of(ctx * strip, strip), strip)
    loads = [
        pltpu.make_async_copy(weight_hbm.at[mine, columns(k)], share.at[k - 1], load_sem.at[k])
        for k in range(1, experts)
    ]
    first_rows = pl.ds(pl.multiple_of(ctx * tokens, tokens), tokens)
    inputs = [
        pltpu.make_async_copy(src, dst, load_sem.at[experts + n])
        for n, (src, dst) in enumerate((
            (key_hbm, keys.at[first_rows, :]), (value_hbm, values.at[first_rows, :]), (query_hbm, query), (hidden_hbm, hidden)
        ))
    ]
    for load in inputs:
        load.start()
    own_load = pltpu.make_async_copy(weight_hbm.at[:, columns(0)], own_weight, load_sem.at[0])
    for load in loads:
        load.start()
    own_load.start()
    greet([partner, near[1], near[2]] + peers)

    sent = []

    def begin(src, dst, send_sem, recv_sem, device):
        copy = remote(src, dst, send_sem, recv_sem, device)
        copy.start()
        sent.append(copy)

    def arrive(view, recv_sem):
        remote(view, view, att_send.at[0], recv_sem, partner).wait_recv()

    def block(i, j, which):
        size = tokens if i < 2 else strip
        owner = mixed(chip, j) * 2 + which
        return pl.ds(pl.multiple_of(owner * size, size), size)

    def half(i, j):
        size = arrays[i].shape[1] // 2
        return pl.ds((j - 1) * size, size)

    def spread(i):
        here = arrays[i].at[block(i, 0, core), :]
        for j in (1, 2):
            begin(here, here, near_send.at[i, j - 1], near_recv.at[i, j - 1], near[j])
        begin(here, here, pair_send.at[i, 0], pair_recv.at[i, 0], partner)

    def forward(i):
        for j in (1, 2):
            here = arrays[i].at[block(i, j, core), :]
            arrive(here, near_recv.at[i, j - 1])
            part = arrays[i].at[block(i, j, core), half(i, j)]
            begin(part, part, half_send.at[i, j - 1], half_recv.at[i, j - 1], near[3 - j])
            begin(here, here, pair_send.at[i, j], pair_recv.at[i, j], partner)

    def corner(i):
        for j in (1, 2):
            arrive(arrays[i].at[block(i, 3, core), half(i, j)], half_recv.at[i, j - 1])
        here = arrays[i].at[block(i, 3, core), :]
        begin(here, here, pair_send.at[i, 3], pair_recv.at[i, 3], partner)

    def passed(i, j):
        arrive(arrays[i].at[block(i, j, 1 - core), :], pair_recv.at[i, j])

    state = [None] * heads

    def attend_chip(j):
        count = 2 * tokens
        start = mixed(chip, j) * count
        rows = pl.ds(pl.multiple_of(start, count), count)
        query_pos = ctx * tokens + lax.broadcasted_iota(jnp.int32, (tokens, count), 0)
        key_pos = start + lax.broadcasted_iota(jnp.int32, (tokens, count), 1)
        visible = key_pos <= query_pos
        for h in range(heads):
            cols = pl.ds(h * HEAD_DIM, HEAD_DIM)
            scores = times_transposed(query[:, cols], keys[rows, cols]) * HEAD_DIM ** (-0.5)
            scores = jnp.where(visible, scores, masked_score)
            top = jnp.max(scores, axis=1, keepdims=True)
            if state[h] is not None:
                top = jnp.maximum(top, state[h][0])
            weights = jnp.where(visible, jnp.exp(scores - top), 0.0)
            total = jnp.sum(weights, axis=1, keepdims=True)
            part = jnp.dot(weights.astype(jnp.bfloat16), values[rows, cols], preferred_element_type=jnp.float32)
            if state[h] is not None:
                fade = jnp.exp(state[h][0] - top)
                total = total + state[h][1] * fade
                part = part + state[h][2] * fade
            state[h] = (top, total, part)

    inputs[0].wait()
    spread(0)
    inputs[1].wait()
    spread(1)
    for k in range(1, experts):
        loads[k - 1].wait()
        begin(share.at[k - 1], walls.at[k - 1, mine, :], share_send.at[k], share_recv.at[k], peers[k - 1])

    def take_share(k):
        arrive(walls.at[k - 1, mine, :], share_recv.at[k])
        spread(k + 1)

    passed(0, 0)
    passed(1, 0)
    inputs[2].wait()
    attend_chip(0)
    forward(0)
    forward(1)
    take_share(1)
    for j in (1, 2):
        passed(0, j)
        passed(1, j)
        attend_chip(j)
    take_share(2)
    corner(0)
    corner(1)
    passed(0, 3)
    passed(1, 3)
    attend_chip(3)
    for h in range(heads):
        att[0, :, h * HEAD_DIM:(h + 1) * HEAD_DIM] = (state[h][2] / state[h][1]).astype(jnp.bfloat16)
    for k in range(1, experts):
        begin(att.at[0], att.at[k], att_send.at[k], att_recv.at[k], peers[k - 1])
    forward(2)
    take_share(3)
    forward(3)
    corner(2)
    forward(4)
    inputs[3].wait()
    total = hidden[...].astype(jnp.float32)
    own_load.wait()
    total = total + jnp.dot(att[0], own_weight[...], preferred_element_type=jnp.float32)
    for k in range(2, experts):
        corner(k + 1)
    for k in range(1, experts):
        for j in range(chips):
            passed(k + 1, j)
        arrive(att.at[k], att_recv.at[k])
        total = total + jnp.dot(att[k], walls[k - 1], preferred_element_type=jnp.float32)
    out[...] = total.astype(jnp.bfloat16)
    for copy in sent:
        copy.wait_send()


def attend_project(experts, query, key, value, hidden, weight):
    tokens, width = hidden.shape
    depth = query.shape[1]
    chips = 4
    strip = depth // (chips * 2)
    bf16 = jnp.bfloat16
    dma = pltpu.SemaphoreType.DMA
    vmem = pl.BlockSpec(memory_space=pltpu.VMEM)
    hbm = pl.BlockSpec(memory_space=pl.ANY)
    return pl.pallas_call(
        functools.partial(attend_kernel, experts),
        out_shape=jax.ShapeDtypeStruct((tokens, width), bf16),
        in_specs=[hbm] * 5,
        out_specs=vmem,
        scratch_shapes=[
            pltpu.VMEM((tokens, depth), bf16),
            pltpu.VMEM((tokens, width), bf16),
            pltpu.VMEM((chips * 2 * tokens, depth), bf16),
            pltpu.VMEM((chips * 2 * tokens, depth), bf16),
            pltpu.VMEM((experts - 1, strip, width), bf16),
            pltpu.VMEM((depth, width), bf16),
            pltpu.VMEM((experts - 1, depth, width), bf16),
            pltpu.VMEM((experts, tokens, depth), bf16),
            dma((experts + 4,)),
            dma((experts + 1, 2)),
            dma((experts + 1, 2)),
            dma((experts + 1, 2)),
            dma((experts + 1, 2)),
            dma((experts + 1, 4)),
            dma((experts + 1, 4)),
            dma((experts,)),
            dma((experts,)),
            dma((experts,)),
            dma((experts,)),
        ],
        compiler_params=pltpu.CompilerParams(
            collective_id=4, has_side_effects=True, vmem_limit_bytes=67043328
        ),
        name="attend_project",
    )(query, key, value, hidden, weight)


def attend(query_heads, key_rows, value_rows, query_offset):
    head_count, row_count, head_width = query_heads.shape
    key_count = key_rows.shape[0]
    key_split = key_rows.reshape(key_count, head_count, head_width)
    value_split = value_rows.reshape(key_count, head_count, head_width)
    scores = jnp.einsum(
        "hqd,khd->hqk", query_heads, key_split, preferred_element_type=jnp.float32
    ) * HEAD_DIM ** (-0.5)
    query_pos = query_offset + lax.broadcasted_iota(jnp.int32, (row_count, key_count), 0)
    key_pos = lax.broadcasted_iota(jnp.int32, (row_count, key_count), 1)
    visible = key_pos <= query_pos
    scores = jnp.where(visible[None], scores, masked_score)
    top = jnp.max(scores, axis=2)
    weights = jnp.where(visible[None], jnp.exp(scores - top[..., None]), 0.0)
    weighted = jnp.einsum(
        "hqk,khd->hqd",
        weights.astype(jnp.bfloat16),
        value_split,
        preferred_element_type=jnp.float32,
    )
    return weighted / jnp.sum(weights, axis=2)[..., None]


def local(
    hidden_in,
    query_vectors,
    key_vectors,
    value_vectors,
    out_weight,
    norm_gain,
    gate_proj,
    up_proj,
    down_proj,
    expert_ids,
    gate_scale,
):
    row_count, local_width = hidden_in.shape
    head_count = query_vectors.shape[1] // HEAD_DIM
    chips = lax.axis_size("ctx") // 2
    expert_count = lax.axis_size("exp")
    capacity = min(row_count, 5 * row_count // (2 * expert_count))
    capacity = -(-capacity // 16) * 16
    if chips == 4 and expert_count == 4:
        residual = attend_project(
            expert_count, query_vectors, key_vectors, value_vectors, hidden_in, out_weight
        )
        return run_square_experts(
            expert_count,
            capacity,
            residual,
            expert_ids.T,
            gate_scale.T,
            norm_gain.reshape(expert_count, 1, local_width),
            gate_proj.transpose(0, 2, 1),
            up_proj.transpose(0, 2, 1),
            down_proj,
        )
    query_heads = query_vectors.reshape(row_count, head_count, HEAD_DIM).transpose(1, 0, 2)
    keys, values = gather_blocks(chips, key_vectors, value_vectors)
    attended = (
        attend(query_heads, keys, values, lax.axis_index("ctx") * row_count)
        .transpose(1, 0, 2)
        .reshape(row_count, head_count * HEAD_DIM)
        .astype(jnp.bfloat16)
    )
    flat_ids = jnp.bitwise_xor(expert_ids.reshape(row_count * 2), lax.axis_index("exp"))
    onehot = (
        flat_ids[:, None] == lax.broadcasted_iota(jnp.int32, (row_count * 2, expert_count), 1)
    ).astype(jnp.int32)
    earlier = jnp.cumsum(onehot, axis=0) - onehot
    slot_index = jnp.sum(earlier * onehot, axis=1)
    target = flat_ids * capacity + slot_index
    placing = (
        target[None, :]
        == lax.broadcasted_iota(jnp.int32, (expert_count * capacity, row_count * 2), 0)
    ).astype(jnp.bfloat16)
    placing_tokens = jnp.sum(placing.reshape(expert_count * capacity, row_count, 2), axis=2)
    residual = project(expert_count, attended, out_weight, hidden_in)
    buffer = jnp.dot(placing_tokens, residual, preferred_element_type=jnp.float32).astype(
        jnp.bfloat16
    )
    returned = run_experts(
        chips,
        expert_count,
        buffer.reshape(expert_count, capacity, local_width),
        norm_gain.reshape(expert_count, 1, local_width),
        gate_proj.transpose(0, 2, 1),
        up_proj.transpose(0, 2, 1),
        down_proj,
    ).reshape(expert_count * capacity, local_width)
    gathered_back = lax.dot_general(
        placing, returned, (((0,), (0,)), ((), ())), preferred_element_type=jnp.float32
    )
    gathered_back = gathered_back.reshape(row_count, 2, local_width)
    combined = (
        residual.astype(jnp.float32)
        + gate_scale[:, 0:1] * gathered_back[:, 0]
        + gate_scale[:, 1:2] * gathered_back[:, 1]
    )
    return combined.astype(jnp.bfloat16)


def solution(mesh):
    placed = (
        P("ctx", "exp"),
        P("ctx", "exp"),
        P("ctx", "exp"),
        P("ctx", "exp"),
        P("exp", None),
        P(),
        P("exp", None, "ctx"),
        P("exp", None, "ctx"),
        P("exp", "ctx", None),
        P("ctx", None),
        P("ctx", None),
    )
    return jax.shard_map(
        local, mesh=mesh, in_specs=placed, out_specs=P("ctx", "exp"), check_vma=False
    )
```

```python
import functools

import jax
import jax.numpy as jnp
from jax import lax
from jax.experimental import pallas as pl
from jax.experimental.pallas import tpu as pltpu
from jax.sharding import PartitionSpec as P

HEAD_DIM = 128
MESH = pl.DeviceIdType.MESH

epsilon = 1e-05
masked_score = -1e30
PIECES = 4


def mixed(index, flip):
    result = index
    bit = 1
    while bit <= flip:
        if flip & bit:
            result = result + bit - 2 * bit * ((index // bit) % 2)
        bit *= 2
    return result


def remote(src, dst, send_sem, recv_sem, device):
    return pltpu.make_async_remote_copy(
        src_ref=src, dst_ref=dst, send_sem=send_sem, recv_sem=recv_sem,
        device_id=device, device_id_type=MESH,
    )


def greet(devices):
    barrier = pltpu.get_barrier_semaphore()
    for device in devices:
        pl.semaphore_signal(barrier, inc=1, device_id=device, device_id_type=MESH)
    pl.semaphore_wait(barrier, len(devices))


def gather_kernel(chips, k_ref, v_ref, ko_ref, vo_ref, local_sem, send_sem, pass_sem, recv_sem, half_send, half_recv):
    ctx, exp = lax.axis_index("ctx"), lax.axis_index("exp")
    chip, core = ctx // 2, ctx % 2
    rows = k_ref.shape[0]
    partner = (chip * 2 + 1 - core, exp)
    others = [(((chip + j) % chips) * 2 + core, exp) for j in range(1, chips)]
    pairs = ((k_ref, ko_ref), (v_ref, vo_ref))
    width = k_ref.shape[1]
    square = chips == 4
    near = (1, 2) if square else tuple(range(chips - 1, 0, -1))

    def device_of(j):
        return (mixed(chip, j) * 2 + core, exp) if square else others[j - 1]

    def source_of(j):
        return mixed(chip, j) if square else (chip + chips - j) % chips

    def half(ref, owner, which):
        part = pl.ds(pl.multiple_of(owner * rows, rows), rows)
        return ref.at[part, pl.ds(which * (width // 2), width // 2)]

    def block(ref, owner):
        return ref.at[pl.ds(pl.multiple_of(owner * rows, rows), rows), :]

    own = []
    for i, (src, dst) in enumerate(pairs):
        own.append(pltpu.make_async_copy(src, block(dst, ctx), local_sem.at[i]))
        own[-1].start()
    greet([partner] + others)
    sent = []
    for i, (src, dst) in enumerate(pairs):
        for j in near:
            sent.append(remote(src, block(dst, ctx), send_sem.at[i, j], recv_sem.at[i, ctx], device_of(j)))
            sent[-1].start()
        sent.append(remote(src, block(dst, ctx), send_sem.at[i, 0], recv_sem.at[i, ctx], partner))
        sent[-1].start()
    for i, (src, dst) in enumerate(pairs):
        for j in near:
            owner = source_of(j) * 2 + core
            here = block(dst, owner)
            passed = remote(here, here, pass_sem.at[i, j], recv_sem.at[i, owner], partner)
            passed.wait_recv()
            if square:
                piece = half(dst, owner, j - 1)
                sent.append(remote(piece, piece, half_send.at[i, j - 1], half_recv.at[i, j - 1], device_of(3 - j)))
                sent[-1].start()
            passed.start()
            sent.append(passed)
    for i, (src, dst) in enumerate(pairs):
        if square:
            owner = mixed(chip, 3) * 2 + core
            for h in range(2):
                piece = half(dst, owner, h)
                remote(piece, piece, half_send.at[i, h], half_recv.at[i, h], partner).wait_recv()
            here = block(dst, owner)
            sent.append(remote(here, here, pass_sem.at[i, 3], recv_sem.at[i, owner], partner))
            sent[-1].start()
    for i, (src, dst) in enumerate(pairs):
        for j in range(chips):
            owner = ((chip + chips - j) % chips) * 2 + 1 - core
            here = block(dst, owner)
            remote(here, here, pass_sem.at[i, 0], recv_sem.at[i, owner], partner).wait_recv()
    for copy in sent:
        copy.wait_send()
    for copy in own:
        copy.wait()


def gather_blocks(chips, keys, values):
    rows, width = keys.shape
    whole = jax.ShapeDtypeStruct((rows * chips * 2, width), keys.dtype)
    return pl.pallas_call(
        functools.partial(gather_kernel, chips),
        out_shape=(whole, whole),
        in_specs=[pl.BlockSpec(memory_space=pltpu.VMEM)] * 2,
        out_specs=[pl.BlockSpec(memory_space=pltpu.VMEM)] * 2,
        scratch_shapes=[
            pltpu.SemaphoreType.DMA((2,)),
            pltpu.SemaphoreType.DMA((2, chips)),
            pltpu.SemaphoreType.DMA((2, chips)),
            pltpu.SemaphoreType.DMA((2, chips * 2)),
            pltpu.SemaphoreType.DMA((2, 2)),
            pltpu.SemaphoreType.DMA((2, 2)),
        ],
        compiler_params=pltpu.CompilerParams(collective_id=0, has_side_effects=True),
        name="gather_blocks",
    )(keys, values)


def project_kernel(experts, att_ref, weight_ref, hidden_ref, out_ref, terms, landed, send_sem, recv_sem):
    ctx, exp = lax.axis_index("ctx"), lax.axis_index("exp")
    width = hidden_ref.shape[1]
    levels = experts.bit_length() - 1
    depth = hidden_ref.shape[0] // PIECES
    peers = [(ctx, mixed(exp, 1 << b)) for b in range(levels)]
    greet(peers)
    sent = []

    def slot(level, k):
        return sum(experts >> (b + 1) for b in range(level)) + k // (2 << level)

    def send(level, k, piece):
        to = slot(level, k - (1 << level))
        here = pl.ds(piece * depth, depth)
        sent.append(remote(
            terms.at[k, here], landed.at[to, here], send_sem.at[to, piece], recv_sem.at[to, piece], peers[level]
        ))
        sent[-1].start()

    order = [k for k in range(experts - 1, -1, -1) if k % 2] + [k for k in range(experts - 1, -1, -1) if not k % 2]
    for k in order:
        columns = pl.ds(pl.multiple_of(mixed(exp, k) * width, width), width)
        terms[k] = jnp.dot(
            att_ref[...], weight_ref[:, columns], preferred_element_type=jnp.float32
        ).astype(jnp.bfloat16)
        if k % 2:
            for piece in range(PIECES):
                send(0, k, piece)
    for level in range(levels):
        for k in range(experts - (2 << level), -1, -(2 << level)):
            at = slot(level, k)
            for piece in range(PIECES):
                here = pl.ds(piece * depth, depth)
                view = landed.at[at, here]
                remote(view, view, send_sem.at[at, piece], recv_sem.at[at, piece], peers[level]).wait_recv()
                total = terms[k, here, :].astype(jnp.float32) + landed[at, here, :].astype(jnp.float32)
                if level + 1 < levels:
                    terms[k, here, :] = total.astype(jnp.bfloat16)
                    if k & (2 << level):
                        send(level + 1, k, piece)
                else:
                    out_ref[here, :] = (hidden_ref[here, :].astype(jnp.float32) + total).astype(jnp.bfloat16)
    for copy in sent:
        copy.wait_send()


def project(experts, attended, weight, hidden):
    rows, width = hidden.shape
    return pl.pallas_call(
        functools.partial(project_kernel, experts),
        out_shape=jax.ShapeDtypeStruct((rows, width), jnp.bfloat16),
        in_specs=[pl.BlockSpec(memory_space=pltpu.VMEM)] * 3,
        out_specs=pl.BlockSpec(memory_space=pltpu.VMEM),
        scratch_shapes=[
            pltpu.VMEM((experts, rows, width), jnp.bfloat16),
            pltpu.VMEM((experts - 1, rows, width), jnp.bfloat16),
            pltpu.SemaphoreType.DMA((experts - 1, PIECES)),
            pltpu.SemaphoreType.DMA((experts - 1, PIECES)),
        ],
        compiler_params=pltpu.CompilerParams(
            collective_id=1, has_side_effects=True, vmem_limit_bytes=32 * 1024 * 1024
        ),
        name="project_reduce",
    )(attended, weight, hidden)


def tiles(width, body, size=256):
    full = width // size
    if full:
        @pl.loop(0, full)
        def _(t):
            body(pl.ds(pl.multiple_of(t * size, size), size))
    if width % size:
        body(pl.ds(full * size, width % size))


def times_transposed(left, right):
    return lax.dot_general(
        left, right, (((1,), (1,)), ((), ())), preferred_element_type=jnp.float32
    )


def experts_kernel(
    chips, experts, buf, gain, gate_hbm, up_hbm, down_hbm, out,
    rows_all, wg, wu, wd, acc_g, acc_u, scaled, hidden, squares, pair_in, chip_in, final,
    w_sem, local_sem, a2a_send, ag_send, pass_send, ag_recv,
    pair_send, pair_recv, rs_send, rs_recv, ret_send, ret_recv,
):
    ctx, exp = lax.axis_index("ctx"), lax.axis_index("exp")
    chip, core = ctx // 2, ctx % 2
    cap, width = buf.shape[1:]
    total_rows = chips * 2 * cap
    features = gate_hbm.shape[2]
    inner = gate_hbm.shape[1]
    partner = (chip * 2 + 1 - core, exp)
    others = [(((chip + j) % chips) * 2 + core, exp) for j in range(1, chips)]
    peers = [(ctx, mixed(exp, k)) for k in range(1, experts)]

    loads = []
    for k in range(experts):
        part = pl.ds(pl.multiple_of(mixed(exp, k) * width, width), width)
        loads.append((
            pltpu.make_async_copy(gate_hbm.at[0, :, part], wg.at[k], w_sem.at[0, k]),
            pltpu.make_async_copy(up_hbm.at[0, :, part], wu.at[k], w_sem.at[1, k]),
        ))
    downs = []
    for k in range(experts):
        part = pl.ds(pl.multiple_of(mixed(exp, k) * width, width), width)
        downs.append(pltpu.make_async_copy(down_hbm.at[0, :, part], wd.at[k], w_sem.at[2, k]))

    def span(index):
        return pl.ds(pl.multiple_of(index * cap, cap), cap)

    mine = core * chips + chip

    own = pltpu.make_async_copy(buf.at[0], rows_all.at[0, span(mine), :], local_sem.at[0])
    own.start()
    for gate_load, up_load in loads:
        gate_load.start()
        up_load.start()
    for k in range(experts - 1, -1, -1):
        downs[k].start()
    greet([partner] + others + peers)

    sent = []
    for k in range(1, experts):
        copy = remote(buf.at[k], rows_all.at[k, span(mine), :], a2a_send.at[k], ag_recv.at[k, mine], peers[k - 1])
        copy.start()
        sent.append(copy)

    def spread(k):
        here = rows_all.at[k, span(mine), :]
        if k == 0:
            own.wait()
        else:
            remote(here, here, a2a_send.at[k], ag_recv.at[k, mine], partner).wait_recv()
        for j in range(chips - 1, 0, -1):
            copy = remote(here, here, ag_send.at[k, j], ag_recv.at[k, mine], others[j - 1])
            copy.start()
            sent.append(copy)
        copy = remote(here, here, ag_send.at[k, 0], ag_recv.at[k, mine], partner)
        copy.start()
        sent.append(copy)

    def collect(k):
        for j in range(1, chips):
            owner = core * chips + (chip + chips - j) % chips
            here = rows_all.at[k, span(owner), :]
            copy = remote(here, here, pass_send.at[k, j], ag_recv.at[k, owner], partner)
            copy.wait_recv()
            copy.start()
            sent.append(copy)
        for j in range(chips):
            owner = (1 - core) * chips + (chip + chips - j) % chips
            here = rows_all.at[k, span(owner), :]
            remote(here, here, pass_send.at[k, 0], ag_recv.at[k, owner], partner).wait_recv()

    spread(0)
    spread(1)
    for k in range(experts):
        collect(k)
        if k + 2 < experts:
            spread(k + 2)
        gain_row = gain[mixed(exp, k)]

        @pl.loop(0, chips * 2)
        def _(b, k=k, gain_row=gain_row):
            x = rows_all[k, span(b), :].astype(jnp.float32)
            square = jnp.broadcast_to(jnp.sum(x * x, axis=1, keepdims=True), (cap, 128))
            squares[span(b), :] = square if k == 0 else squares[span(b), :] + square
            scaled[span(b), :] = (x * gain_row).astype(jnp.bfloat16)

        loads[k][0].wait()
        loads[k][1].wait()
        last = k == experts - 1
        if last:
            squares[...] = lax.rsqrt(squares[...] * (1.0 / features) + epsilon)

        def up_tile(cols, k=k, last=last):
            g = times_transposed(scaled[...], wg[k, cols, :])
            u = times_transposed(scaled[...], wu[k, cols, :])
            if k:
                g = g + acc_g[:, cols]
                u = u + acc_u[:, cols]
            if last:
                inverse = squares[:, 0:1]
                g = g * inverse
                u = u * inverse
                hidden[:, cols] = (g / (1.0 + jnp.exp(-g)) * u).astype(jnp.bfloat16)
            else:
                acc_g[:, cols] = g
                acc_u[:, cols] = u

        tiles(inner, up_tile)

    for copy in sent:
        copy.wait_send()
    sent = []
    half = chips * cap

    def half_of(which):
        return pl.ds(pl.multiple_of(which * half, half), half)

    def multiply(k):
        downs[k].wait()

        def down_tile(cols):
            rows_all[k, :, cols] = jnp.dot(
                hidden[...], wd[k, :, cols], preferred_element_type=jnp.float32
            ).astype(jnp.bfloat16)

        tiles(width, down_tile)
        copy = remote(rows_all.at[k, half_of(1 - core), :], pair_in.at[k], pair_send.at[k], pair_recv.at[k], partner)
        copy.start()
        sent.append(copy)

    def merge(k):
        remote(pair_in.at[k], pair_in.at[k], pair_send.at[k], pair_recv.at[k], partner).wait_recv()
        for j in range(chips - 1, -1, -1):
            to = (chip + j) % chips
            place = span(core * chips + to)
            rows_all[k, place, :] = (
                rows_all[k, place, :].astype(jnp.float32) + pair_in[k, span(to), :].astype(jnp.float32)
            ).astype(jnp.bfloat16)
            if j:
                copy = remote(rows_all.at[k, place, :], chip_in.at[k, j - 1], rs_send.at[k, j], rs_recv.at[k, j], others[j - 1])
                copy.start()
                sent.append(copy)

    def finish(k):
        value = rows_all[k, span(mine), :].astype(jnp.float32)
        for j in range(1, chips):
            here = chip_in.at[k, j - 1]
            remote(here, here, rs_send.at[k, j], rs_recv.at[k, j], partner).wait_recv()
            value = value + chip_in[k, j - 1].astype(jnp.float32)
        if k == 0:
            out[0] = value.astype(jnp.bfloat16)
        else:
            final[k] = value.astype(jnp.bfloat16)
            copy = remote(final.at[k], out.at[k], ret_send.at[k], ret_recv.at[k], peers[k - 1])
            copy.start()
            sent.append(copy)

    order = list(range(experts - 1, -1, -1))
    for step in range(experts + 2):
        if step < experts:
            multiply(order[step])
        if 1 <= step <= experts:
            merge(order[step - 1])
        if step >= 2:
            finish(order[step - 2])
    for k in range(1, experts):
        remote(out.at[k], out.at[k], ret_send.at[k], ret_recv.at[k], peers[k - 1]).wait_recv()
    for copy in sent:
        copy.wait_send()


def run_experts(chips, experts, buffer, gain, gate, up, down):
    _, cap, width = buffer.shape
    inner = gate.shape[1]
    rows = chips * 2 * cap
    bf16, f32 = jnp.bfloat16, jnp.float32
    dma = pltpu.SemaphoreType.DMA
    vmem = pl.BlockSpec(memory_space=pltpu.VMEM)
    hbm = pl.BlockSpec(memory_space=pl.ANY)
    return pl.pallas_call(
        functools.partial(experts_kernel, chips, experts),
        out_shape=jax.ShapeDtypeStruct((experts, cap, width), bf16),
        in_specs=[vmem, vmem, hbm, hbm, hbm],
        out_specs=vmem,
        scratch_shapes=[
            pltpu.VMEM((experts, rows, width), bf16),
            pltpu.VMEM((experts, inner, width), bf16),
            pltpu.VMEM((experts, inner, width), bf16),
            pltpu.VMEM((experts, inner, width), bf16),
            pltpu.VMEM((rows, inner), f32),
            pltpu.VMEM((rows, inner), f32),
            pltpu.VMEM((rows, width), bf16),
            pltpu.VMEM((rows, inner), bf16),
            pltpu.VMEM((rows, 128), f32),
            pltpu.VMEM((experts, chips * cap, width), bf16),
            pltpu.VMEM((experts, chips - 1, cap, width), bf16),
            pltpu.VMEM((experts, cap, width), bf16),
            dma((3, experts)),
            dma((1,)),
            dma((experts,)),
            dma((experts, chips)),
            dma((experts, chips)),
            dma((experts, chips * 2)),
            dma((experts,)),
            dma((experts,)),
            dma((experts, chips)),
            dma((experts, chips)),
            dma((experts,)),
            dma((experts,)),
        ],
        compiler_params=pltpu.CompilerParams(
            collective_id=2, has_side_effects=True, vmem_limit_bytes=67043328
        ),
        name="experts",
    )(buffer, gain, gate, up, down)


def announce(devices):
    barrier = pltpu.get_barrier_semaphore()
    for device in devices:
        pl.semaphore_signal(barrier, inc=1, device_id=device, device_id_type=MESH)


def admit(devices):
    pl.semaphore_wait(pltpu.get_barrier_semaphore(), len(devices))


def eye_of(rows, columns):
    return lax.broadcasted_iota(jnp.int32, (rows, columns), 0) == lax.broadcasted_iota(jnp.int32, (rows, columns), 1)


def as_row(column, columns):
    rows = column.shape[0]
    return jnp.sum(jnp.where(eye_of(rows, columns), column, 0.0), axis=0, keepdims=True)


def routed(ids_ref, scale_ref, onehot, weigh, cuts, experts, exp):
    tokens = ids_ref.shape[1]
    relative = lax.broadcasted_iota(jnp.int32, (experts, tokens), 0)
    wanted = jnp.bitwise_xor(relative, exp)
    first, second = ids_ref[0:1, :] == wanted, ids_ref[1:2, :] == wanted
    member = (first | second).astype(jnp.float32)
    gates = jnp.where(first, scale_ref[0:1, :], 0.0) + jnp.where(second, scale_ref[1:2, :], 0.0)
    earlier = (
        lax.broadcasted_iota(jnp.int32, (tokens, tokens), 0) < lax.broadcasted_iota(jnp.int32, (tokens, tokens), 1)
    ).astype(jnp.bfloat16)
    place = jnp.dot(member.astype(jnp.bfloat16), earlier, preferred_element_type=jnp.float32)
    place = jnp.where(member > 0.5, place, -1.0).astype(jnp.int32)
    base = 0
    for r, count in enumerate(cuts):
        slots = base + lax.broadcasted_iota(jnp.int32, (count, tokens), 0)
        for k in range(experts):
            chosen = slots == place[k:k + 1, :]
            onehot[k, base:base + count, :] = chosen.astype(jnp.bfloat16)
            gate = jnp.where(chosen, gates[k:k + 1, :], 0.0)
            high = gate.astype(jnp.bfloat16)
            rows = pl.ds(k * count, count)
            weigh[r][0, rows, :] = high
            weigh[r][1, rows, :] = (gate - high.astype(jnp.float32)).astype(jnp.bfloat16)
        base += count


def square_experts_kernel(
    experts, cuts, residual, ids, scale, gain, gate_hbm, up_hbm, down_hbm, out,
    onehot, weigh_a, weigh_b, normal, buf_a, buf_b, rows_a, rows_b, wg, wu, wd, acc_g, acc_u, part_g, part_u, hidden_a, hidden_b,
    pair_a, pair_b, near_a, near_b, far_a, far_b, final_a, final_b, back_a, back_b, summed,
    sums, sums_in, inverse_out, inverse_in, inverse_a, inverse_b,
    w_sem, own_send, own_recv, near_send, near_recv, half_send, half_recv, pair_send, pair_recv,
    swap_send, swap_recv, one_send, one_recv, two_send, two_recv, ret_send, ret_recv,
    sum_send, sum_recv, inv_send, inv_recv,
):
    chips = 4
    ctx, exp = lax.axis_index("ctx"), lax.axis_index("exp")
    chip, core = ctx // 2, ctx % 2
    tokens, width = residual.shape
    features = gate_hbm.shape[2]
    inner = gate_hbm.shape[1]
    wing = width // 2
    cap = sum(cuts)
    weigh, buf, rows = (weigh_a, weigh_b), (buf_a, buf_b), (rows_a, rows_b)
    hidden, pair_in, near_in, far_in = (hidden_a, hidden_b), (pair_a, pair_b), (near_a, near_b), (far_a, far_b)
    final, back, inverse = (final_a, final_b), (back_a, back_b), (inverse_a, inverse_b)
    partner = (chip * 2 + 1 - core, exp)
    near = {j: (mixed(chip, j) * 2 + core, exp) for j in (1, 2)}
    peers = [(ctx, mixed(exp, k)) for k in range(1, experts)]
    plane = [(mixed(chip, j) * 2 + mixed(core, c), exp) for j in range(chips) for c in range(2)][1:]

    def f32(value):
        return value.astype(jnp.float32)

    def chunk(k):
        return pl.ds(k * width, width)

    loads, downs = [], []
    for k in range(experts):
        part = pl.ds(pl.multiple_of(mixed(exp, k) * width, width), width)
        loads.append((
            pltpu.make_async_copy(gate_hbm.at[0, :, part], wg.at[:, chunk(k)], w_sem.at[0, k]),
            pltpu.make_async_copy(up_hbm.at[0, :, part], wu.at[:, chunk(k)], w_sem.at[1, k]),
        ))
        downs.append(pltpu.make_async_copy(down_hbm.at[0, :, part], wd.at[k], w_sem.at[2, k]))
    for gate_load, up_load in loads:
        gate_load.start()
        up_load.start()
    for k in range(experts - 1, -1, -1):
        downs[k].start()

    def block(j, which):
        return which * chips + mixed(chip, j)

    def span(r, index):
        return pl.ds(pl.multiple_of(index * cuts[r], cuts[r]), cuts[r])

    def wings(k, way):
        return pl.ds(k * width + (way - 1) * wing, wing)

    mine = block(0, core)
    started = {"sums": [], 0: [], 1: [], "back": []}

    def begin(group, src, dst, send_sem, recv_sem, device):
        copy = remote(src, dst, send_sem, recv_sem, device)
        copy.start()
        started[group].append(copy)

    def arrive(view, recv_sem):
        remote(view, view, sum_send.at[0], recv_sem, partner).wait_recv()

    def settle(group):
        for copy in started[group]:
            copy.wait_send()
        started[group].clear()

    announce(plane + peers)
    routed(ids, scale, onehot, weigh, cuts, experts, exp)

    def prepare():
        x = f32(residual[...])
        normal[...] = (x * gain[exp]).astype(jnp.bfloat16)
        total = as_row(jnp.sum(x * x, axis=1, keepdims=True), tokens)
        sums[...] = jnp.broadcast_to(total, sums.shape)

    def route(r, k):
        base = sum(cuts[:r])
        picked = jnp.dot(
            onehot[k, base:base + cuts[r], :], normal[...], preferred_element_type=jnp.float32
        ).astype(jnp.bfloat16)
        if k == 0:
            rows[r][span(r, mine), chunk(0)] = picked
        else:
            buf[r][k] = picked

    def deliver(r):
        for k in range(1, experts):
            begin(r, buf[r].at[k], rows[r].at[span(r, mine), chunk(k)], own_send.at[r, k], own_recv.at[r, k], peers[k - 1])

    def spread(r, k):
        here = rows[r].at[span(r, mine), chunk(k)]
        if k:
            arrive(here, own_recv.at[r, k])
        for j in (1, 2):
            begin(r, here, here, near_send.at[r, k, j], near_recv.at[r, k, j], near[j])
        begin(r, here, here, pair_send.at[r, k, 0], pair_recv.at[r, k, 0], partner)

    def forward(r, k):
        for j in (1, 2):
            place = span(r, block(j, core))
            here = rows[r].at[place, chunk(k)]
            arrive(here, near_recv.at[r, k, j])
            part = rows[r].at[place, wings(k, j)]
            begin(r, part, part, half_send.at[r, k, j], half_recv.at[r, k, j], near[3 - j])
            begin(r, here, here, pair_send.at[r, k, j], pair_recv.at[r, k, j], partner)

    def corner(r, k):
        place = span(r, block(3, core))
        for j in (1, 2):
            arrive(rows[r].at[place, wings(k, j)], half_recv.at[r, k, j])
        here = rows[r].at[place, chunk(k)]
        begin(r, here, here, pair_send.at[r, k, 3], pair_recv.at[r, k, 3], partner)

    def gathered(r, k):
        for j in range(chips):
            arrive(rows[r].at[span(r, block(j, 1 - core)), chunk(k)], pair_recv.at[r, k, j])
        if r == 0:
            loads[k][0].wait()
            loads[k][1].wait()

    def share_sums():
        for k in range(1, experts):
            begin("sums", sums, sums_in.at[k], sum_send.at[k], sum_recv.at[k], peers[k - 1])

    def share_inverse():
        total = sums[...]
        for k in range(1, experts):
            arrive(sums_in.at[k], sum_recv.at[k])
            total = total + sums_in[k]
        value = lax.rsqrt(total * (1.0 / features) + epsilon)[0:1, :]
        column = jnp.sum(jnp.where(onehot[0] > 0.5, value, 0.0), axis=1, keepdims=True)
        row = as_row(column, inverse_out.shape[1])
        inverse_out[...] = jnp.broadcast_to(row, inverse_out.shape)
        inverse_in[mine] = jnp.broadcast_to(row, inverse_out.shape)
        for n, device in enumerate(plane):
            begin("sums", inverse_out, inverse_in.at[mine], inv_send.at[n], inv_recv.at[mine], device)

    def take_inverse():
        for j in range(chips):
            for which in range(2):
                if j or which:
                    index = block(j, mixed(core, which))
                    arrive(inverse_in.at[index], inv_recv.at[index])
        for b in range(chips * 2):
            row = inverse_in[b][0:1, :]
            column = jnp.sum(jnp.where(eye_of(cap, row.shape[1]), row, 0.0), axis=1, keepdims=True)
            column = jnp.broadcast_to(column, (cap, 128))
            base = 0
            for r, count in enumerate(cuts):
                inverse[r][b * count:(b + 1) * count, :] = column[base:base + count, :]
                base += count

    def activate(r, at, g, u):
        by = inverse[r][:, 0:1]
        g = g * by
        u = u * by
        hidden[r][:, at] = (g / (1.0 + jnp.exp(-g)) * u).astype(jnp.bfloat16)

    tile = 512
    body = inner // tile * tile

    def up_tile(k):
        def one(at):
            g = times_transposed(rows_a[:, chunk(k)], wg[at, chunk(k)])
            u = times_transposed(rows_a[:, chunk(k)], wu[at, chunk(k)])
            if k:
                g = g + acc_g[:, at]
                u = u + acc_u[:, at]
            if k == experts - 1:
                activate(0, at, g, u)
            else:
                acc_g[:, at] = g
                acc_u[:, at] = u
        return one

    def expand_first(k):
        gathered(0, k)
        if k == experts - 1:
            take_inverse()
        if body:
            tiles(body, up_tile(k), tile)

    def expand_rest(k):
        if inner > body:
            up_tile(k)(pl.ds(body, inner - body))

    def whole_tile(at):
        rest = pl.ds(width, (experts - 1) * width)
        g = times_transposed(rows_b[:, rest], wg[at, rest]) + part_g[:, at]
        u = times_transposed(rows_b[:, rest], wu[at, rest]) + part_u[:, at]
        activate(1, at, g, u)

    def expand_part():
        gathered(1, 0)

        def one(at):
            part_g[:, at] = times_transposed(rows_b[:, chunk(0)], wg[at, chunk(0)])
            part_u[:, at] = times_transposed(rows_b[:, chunk(0)], wu[at, chunk(0)])

        tiles(inner, one, tile)

    def multiply(r, k):
        if r == 0:
            downs[k].wait()
        rows[r][:, chunk(k)] = jnp.dot(
            hidden[r][...], wd[k], preferred_element_type=jnp.float32
        ).astype(jnp.bfloat16)
        half = chips * cuts[r]
        there = pl.ds(pl.multiple_of((1 - core) * half, half), half)
        begin("back", rows[r].at[there, chunk(k)], pair_in[r].at[k], swap_send.at[r, k], swap_recv.at[r, k], partner)

    def paired(r, k, j, way):
        inside = pl.ds((way - 1) * wing, wing)
        return f32(rows[r][span(r, block(j, core)), wings(k, way)]) + f32(pair_in[r][k, span(r, mixed(chip, j)), inside])

    def merge(r, k):
        arrive(pair_in[r].at[k], swap_recv.at[r, k])
        for way in (1, 2):
            for slot, j in ((1, 3), (0, way)):
                here = (span(r, block(j, core)), wings(k, way))
                rows[r][here] = paired(r, k, j, way).astype(jnp.bfloat16)
                begin(
                    "back", rows[r].at[here], near_in[r].at[k, way - 1, slot],
                    one_send.at[r, k, way - 1, slot], one_recv.at[r, k, way - 1, slot], near[way],
                )

    def relay(r, k):
        for way in (1, 2):
            arrive(near_in[r].at[k, way - 1, 1], one_recv.at[r, k, way - 1, 1])
            j = 3 - way
            value = paired(r, k, j, way) + f32(near_in[r][k, way - 1, 1])
            here = (span(r, block(j, core)), wings(k, way))
            rows[r][here] = value.astype(jnp.bfloat16)
            begin(
                "back", rows[r].at[here], far_in[r].at[k, way - 1],
                two_send.at[r, k, way - 1], two_recv.at[r, k, way - 1], near[j],
            )

    def finish(r, k):
        for way in (1, 2):
            arrive(near_in[r].at[k, way - 1, 0], one_recv.at[r, k, way - 1, 0])
            arrive(far_in[r].at[k, way - 1], two_recv.at[r, k, way - 1])
            value = paired(r, k, 0, way) + f32(near_in[r][k, way - 1, 0]) + f32(far_in[r][k, way - 1])
            inside = pl.ds((way - 1) * wing, wing)
            if k == 0:
                back[r][0, :, inside] = value.astype(jnp.bfloat16)
            else:
                final[r][k, :, inside] = value.astype(jnp.bfloat16)
        if k:
            begin("back", final[r].at[k], back[r].at[k], ret_send.at[r, k], ret_recv.at[r, k], peers[k - 1])

    def combine(r):
        for k in range(1, experts):
            arrive(back[r].at[k], ret_recv.at[r, k])
        given = back[r][...].reshape(experts * cuts[r], width)
        value = f32(residual[...]) if r == 0 else summed[...]
        for which in range(2):
            value = value + lax.dot_general(
                weigh[r][which], given, (((0,), (0,)), ((), ())), preferred_element_type=jnp.float32
            )
        if r == 0:
            summed[...] = value
        else:
            out[...] = value.astype(jnp.bfloat16)

    prepare()
    for k in range(experts):
        route(0, k)
    route(1, 0)
    admit(plane + peers)
    share_sums()
    spread(0, 0)
    deliver(0)
    spread(1, 0)

    forward(0, 0)
    spread(0, 1)
    corner(0, 0)
    forward(1, 0)
    expand_first(0)
    forward(0, 1)
    spread(0, 2)
    corner(1, 0)
    expand_rest(0)
    for k in range(1, experts):
        route(1, k)
    deliver(1)
    expand_part()
    corner(0, 1)
    forward(0, 2)
    spread(0, 3)
    share_inverse()
    expand_first(1)
    corner(0, 2)
    expand_rest(1)
    forward(0, 3)
    spread(1, 1)
    expand_first(2)
    corner(0, 3)
    forward(1, 1)
    spread(1, 2)
    expand_rest(2)
    expand_first(3)
    corner(1, 1)
    forward(1, 2)
    spread(1, 3)
    expand_rest(3)
    settle(0)
    multiply(0, 3)
    corner(1, 2)
    forward(1, 3)
    multiply(0, 2)
    merge(0, 3)
    multiply(0, 1)
    merge(0, 2)
    corner(1, 3)
    multiply(0, 0)
    merge(0, 1)
    relay(0, 3)
    for k in range(1, experts):
        gathered(1, k)
    merge(0, 0)
    cuts_at = [pl.ds(at, min(tile, inner - at)) for at in range(0, inner, tile)]
    between = [
        ((relay, 2),),
        ((relay, 1), (finish, 3)),
        ((relay, 0), (finish, 2)),
    ]
    for n, at in enumerate(cuts_at):
        whole_tile(at)
        for action, k in between[n] if n < len(between) else ():
            action(0, k)
    for group in between[len(cuts_at):]:
        for action, k in group:
            action(0, k)
    settle(1)
    multiply(1, 3)
    finish(0, 1)
    multiply(1, 2)
    merge(1, 3)
    finish(0, 0)
    multiply(1, 1)
    merge(1, 2)
    multiply(1, 0)
    merge(1, 1)
    relay(1, 3)
    merge(1, 0)
    relay(1, 2)
    finish(1, 3)
    relay(1, 1)
    combine(0)
    finish(1, 2)
    relay(1, 0)
    finish(1, 1)
    finish(1, 0)
    combine(1)
    settle("back")
    settle("sums")


def run_square_experts(experts, cap, residual, ids, scale, gain, gate, up, down):
    tokens, width = residual.shape
    inner = gate.shape[1]
    chips = 4
    first = cap // 16 * 3 // 5 * 16
    cuts = (first, cap - first)
    bf16, f32 = jnp.bfloat16, jnp.float32
    dma = pltpu.SemaphoreType.DMA
    vmem = pl.BlockSpec(memory_space=pltpu.VMEM)
    hbm = pl.BlockSpec(memory_space=pl.ANY)

    def both(shape, dtype=bf16):
        return [pltpu.VMEM(shape(count), dtype) for count in cuts]

    return pl.pallas_call(
        functools.partial(square_experts_kernel, experts, cuts),
        out_shape=jax.ShapeDtypeStruct((tokens, width), bf16),
        in_specs=[vmem, vmem, vmem, vmem, hbm, hbm, hbm],
        out_specs=vmem,
        scratch_shapes=[
            pltpu.VMEM((experts, cap, tokens), bf16),
            *both(lambda n: (2, experts * n, tokens)),
            pltpu.VMEM((tokens, width), bf16),
            *both(lambda n: (experts, n, width)),
            *both(lambda n: (chips * 2 * n, experts * width)),
            pltpu.VMEM((inner, experts * width), bf16),
            pltpu.VMEM((inner, experts * width), bf16),
            pltpu.VMEM((experts, inner, width), bf16),
            pltpu.VMEM((chips * 2 * cuts[0], inner), f32),
            pltpu.VMEM((chips * 2 * cuts[0], inner), f32),
            pltpu.VMEM((chips * 2 * cuts[1], inner), f32),
            pltpu.VMEM((chips * 2 * cuts[1], inner), f32),
            *both(lambda n: (chips * 2 * n, inner)),
            *both(lambda n: (experts, chips * n, width)),
            *both(lambda n: (experts, 2, 2, n, width // 2)),
            *both(lambda n: (experts, 2, n, width // 2)),
            *both(lambda n: (experts, n, width)),
            *both(lambda n: (experts, n, width)),
            pltpu.VMEM((tokens, width), f32),
            pltpu.VMEM((8, tokens), f32),
            pltpu.VMEM((experts, 8, tokens), f32),
            pltpu.VMEM((8, 128), f32),
            pltpu.VMEM((chips * 2, 8, 128), f32),
            *both(lambda n: (chips * 2 * n, 128), f32),
            dma((3, experts)),
            dma((2, experts)),
            dma((2, experts)),
            dma((2, experts, 3)),
            dma((2, experts, 3)),
            dma((2, experts, 3)),
            dma((2, experts, 3)),
            dma((2, experts, 4)),
            dma((2, experts, 4)),
            dma((2, experts)),
            dma((2, experts)),
            dma((2, experts, 2, 2)),
            dma((2, experts, 2, 2)),
            dma((2, experts, 2)),
            dma((2, experts, 2)),
            dma((2, experts)),
            dma((2, experts)),
            dma((experts,)),
            dma((experts,)),
            dma((chips * 2 - 1,)),
            dma((chips * 2,)),
        ],
        compiler_params=pltpu.CompilerParams(
            collective_id=3, has_side_effects=True, vmem_limit_bytes=67043328
        ),
        name="square_experts",
    )(residual, ids, scale, gain, gate, up, down)


def attend_kernel(
    experts, query_hbm, key_hbm, value_hbm, hidden_hbm, weight_hbm, out,
    query, hidden, keys, values, share, own_weight, walls, att,
    load_sem, near_send, near_recv, half_send, half_recv, pair_send, pair_recv,
    share_send, share_recv, att_send, att_recv,
):
    chips = 4
    ctx, exp = lax.axis_index("ctx"), lax.axis_index("exp")
    chip, core = ctx // 2, ctx % 2
    tokens, depth = query.shape
    width = hidden.shape[1]
    heads = depth // HEAD_DIM
    strip = share.shape[1]
    partner = (chip * 2 + 1 - core, exp)
    near = {j: (mixed(chip, j) * 2 + core, exp) for j in (1, 2)}
    peers = [(ctx, mixed(exp, k)) for k in range(1, experts)]
    arrays = [keys, values] + [walls.at[k] for k in range(experts - 1)]

    def columns(k):
        return pl.ds(pl.multiple_of(mixed(exp, k) * width, width), width)

    mine = pl.ds(pl.multiple_of(ctx * strip, strip), strip)
    loads = [
        pltpu.make_async_copy(weight_hbm.at[mine, columns(k)], share.at[k - 1], load_sem.at[k])
        for k in range(1, experts)
    ]
    first_rows = pl.ds(pl.multiple_of(ctx * tokens, tokens), tokens)
    inputs = [
        pltpu.make_async_copy(src, dst, load_sem.at[experts + n])
        for n, (src, dst) in enumerate((
            (key_hbm, keys.at[first_rows, :]), (value_hbm, values.at[first_rows, :]), (query_hbm, query), (hidden_hbm, hidden)
        ))
    ]
    for load in inputs:
        load.start()
    own_load = pltpu.make_async_copy(weight_hbm.at[:, columns(0)], own_weight, load_sem.at[0])
    for load in loads:
        load.start()
    own_load.start()
    greet([partner, near[1], near[2]] + peers)

    sent = []

    def begin(src, dst, send_sem, recv_sem, device):
        copy = remote(src, dst, send_sem, recv_sem, device)
        copy.start()
        sent.append(copy)

    def arrive(view, recv_sem):
        remote(view, view, att_send.at[0], recv_sem, partner).wait_recv()

    def block(i, j, which):
        size = tokens if i < 2 else strip
        owner = mixed(chip, j) * 2 + which
        return pl.ds(pl.multiple_of(owner * size, size), size)

    def half(i, j):
        size = arrays[i].shape[1] // 2
        return pl.ds((j - 1) * size, size)

    def spread(i):
        here = arrays[i].at[block(i, 0, core), :]
        for j in (1, 2):
            begin(here, here, near_send.at[i, j - 1], near_recv.at[i, j - 1], near[j])
        begin(here, here, pair_send.at[i, 0], pair_recv.at[i, 0], partner)

    def forward(i):
        for j in (1, 2):
            here = arrays[i].at[block(i, j, core), :]
            arrive(here, near_recv.at[i, j - 1])
            part = arrays[i].at[block(i, j, core), half(i, j)]
            begin(part, part, half_send.at[i, j - 1], half_recv.at[i, j - 1], near[3 - j])
            begin(here, here, pair_send.at[i, j], pair_recv.at[i, j], partner)

    def corner(i):
        for j in (1, 2):
            arrive(arrays[i].at[block(i, 3, core), half(i, j)], half_recv.at[i, j - 1])
        here = arrays[i].at[block(i, 3, core), :]
        begin(here, here, pair_send.at[i, 3], pair_recv.at[i, 3], partner)

    def passed(i, j):
        arrive(arrays[i].at[block(i, j, 1 - core), :], pair_recv.at[i, j])

    state = [None] * heads

    def attend_chip(j):
        count = 2 * tokens
        start = mixed(chip, j) * count
        rows = pl.ds(pl.multiple_of(start, count), count)
        query_pos = ctx * tokens + lax.broadcasted_iota(jnp.int32, (tokens, count), 0)
        key_pos = start + lax.broadcasted_iota(jnp.int32, (tokens, count), 1)
        visible = key_pos <= query_pos
        for h in range(heads):
            cols = pl.ds(h * HEAD_DIM, HEAD_DIM)
            scores = times_transposed(query[:, cols], keys[rows, cols]) * HEAD_DIM ** (-0.5)
            scores = jnp.where(visible, scores, masked_score)
            top = jnp.max(scores, axis=1, keepdims=True)
            if state[h] is not None:
                top = jnp.maximum(top, state[h][0])
            weights = jnp.where(visible, jnp.exp(scores - top), 0.0)
            total = jnp.sum(weights, axis=1, keepdims=True)
            part = jnp.dot(weights.astype(jnp.bfloat16), values[rows, cols], preferred_element_type=jnp.float32)
            if state[h] is not None:
                fade = jnp.exp(state[h][0] - top)
                total = total + state[h][1] * fade
                part = part + state[h][2] * fade
            state[h] = (top, total, part)

    inputs[0].wait()
    spread(0)
    inputs[1].wait()
    spread(1)
    for k in range(1, experts):
        loads[k - 1].wait()
        begin(share.at[k - 1], walls.at[k - 1, mine, :], share_send.at[k], share_recv.at[k], peers[k - 1])

    def take_share(k):
        arrive(walls.at[k - 1, mine, :], share_recv.at[k])
        spread(k + 1)

    passed(0, 0)
    passed(1, 0)
    inputs[2].wait()
    attend_chip(0)
    forward(0)
    forward(1)
    take_share(1)
    for j in (1, 2):
        passed(0, j)
        passed(1, j)
        attend_chip(j)
    take_share(2)
    corner(0)
    corner(1)
    passed(0, 3)
    passed(1, 3)
    attend_chip(3)
    for h in range(heads):
        att[0, :, h * HEAD_DIM:(h + 1) * HEAD_DIM] = (state[h][2] / state[h][1]).astype(jnp.bfloat16)
    for k in range(1, experts):
        begin(att.at[0], att.at[k], att_send.at[k], att_recv.at[k], peers[k - 1])
    forward(2)
    take_share(3)
    forward(3)
    corner(2)
    forward(4)
    inputs[3].wait()
    total = hidden[...].astype(jnp.float32)
    own_load.wait()
    total = total + jnp.dot(att[0], own_weight[...], preferred_element_type=jnp.float32)
    for k in range(2, experts):
        corner(k + 1)
    for k in range(1, experts):
        for j in range(chips):
            passed(k + 1, j)
        arrive(att.at[k], att_recv.at[k])
        total = total + jnp.dot(att[k], walls[k - 1], preferred_element_type=jnp.float32)
    out[...] = total.astype(jnp.bfloat16)
    for copy in sent:
        copy.wait_send()


def attend_project(experts, query, key, value, hidden, weight):
    tokens, width = hidden.shape
    depth = query.shape[1]
    chips = 4
    strip = depth // (chips * 2)
    bf16 = jnp.bfloat16
    dma = pltpu.SemaphoreType.DMA
    vmem = pl.BlockSpec(memory_space=pltpu.VMEM)
    hbm = pl.BlockSpec(memory_space=pl.ANY)
    return pl.pallas_call(
        functools.partial(attend_kernel, experts),
        out_shape=jax.ShapeDtypeStruct((tokens, width), bf16),
        in_specs=[hbm] * 5,
        out_specs=vmem,
        scratch_shapes=[
            pltpu.VMEM((tokens, depth), bf16),
            pltpu.VMEM((tokens, width), bf16),
            pltpu.VMEM((chips * 2 * tokens, depth), bf16),
            pltpu.VMEM((chips * 2 * tokens, depth), bf16),
            pltpu.VMEM((experts - 1, strip, width), bf16),
            pltpu.VMEM((depth, width), bf16),
            pltpu.VMEM((experts - 1, depth, width), bf16),
            pltpu.VMEM((experts, tokens, depth), bf16),
            dma((experts + 4,)),
            dma((experts + 1, 2)),
            dma((experts + 1, 2)),
            dma((experts + 1, 2)),
            dma((experts + 1, 2)),
            dma((experts + 1, 4)),
            dma((experts + 1, 4)),
            dma((experts,)),
            dma((experts,)),
            dma((experts,)),
            dma((experts,)),
        ],
        compiler_params=pltpu.CompilerParams(
            collective_id=4, has_side_effects=True, vmem_limit_bytes=67043328
        ),
        name="attend_project",
    )(query, key, value, hidden, weight)


def attend(query_heads, key_rows, value_rows, query_offset):
    head_count, row_count, head_width = query_heads.shape
    key_count = key_rows.shape[0]
    key_split = key_rows.reshape(key_count, head_count, head_width)
    value_split = value_rows.reshape(key_count, head_count, head_width)
    scores = jnp.einsum(
        "hqd,khd->hqk", query_heads, key_split, preferred_element_type=jnp.float32
    ) * HEAD_DIM ** (-0.5)
    query_pos = query_offset + lax.broadcasted_iota(jnp.int32, (row_count, key_count), 0)
    key_pos = lax.broadcasted_iota(jnp.int32, (row_count, key_count), 1)
    visible = key_pos <= query_pos
    scores = jnp.where(visible[None], scores, masked_score)
    top = jnp.max(scores, axis=2)
    weights = jnp.where(visible[None], jnp.exp(scores - top[..., None]), 0.0)
    weighted = jnp.einsum(
        "hqk,khd->hqd",
        weights.astype(jnp.bfloat16),
        value_split,
        preferred_element_type=jnp.float32,
    )
    return weighted / jnp.sum(weights, axis=2)[..., None]


def local(
    hidden_in,
    query_vectors,
    key_vectors,
    value_vectors,
    out_weight,
    norm_gain,
    gate_proj,
    up_proj,
    down_proj,
    expert_ids,
    gate_scale,
):
    row_count, local_width = hidden_in.shape
    head_count = query_vectors.shape[1] // HEAD_DIM
    chips = lax.axis_size("ctx") // 2
    expert_count = lax.axis_size("exp")
    capacity = min(row_count, 5 * row_count // (2 * expert_count))
    capacity = -(-capacity // 16) * 16
    if chips == 4 and expert_count == 4:
        residual = attend_project(
            expert_count, query_vectors, key_vectors, value_vectors, hidden_in, out_weight
        )
        return run_square_experts(
            expert_count,
            capacity,
            residual,
            expert_ids.T,
            gate_scale.T,
            norm_gain.reshape(expert_count, 1, local_width),
            gate_proj.transpose(0, 2, 1),
            up_proj.transpose(0, 2, 1),
            down_proj,
        )
    query_heads = query_vectors.reshape(row_count, head_count, HEAD_DIM).transpose(1, 0, 2)
    keys, values = gather_blocks(chips, key_vectors, value_vectors)
    attended = (
        attend(query_heads, keys, values, lax.axis_index("ctx") * row_count)
        .transpose(1, 0, 2)
        .reshape(row_count, head_count * HEAD_DIM)
        .astype(jnp.bfloat16)
    )
    flat_ids = jnp.bitwise_xor(expert_ids.reshape(row_count * 2), lax.axis_index("exp"))
    onehot = (
        flat_ids[:, None] == lax.broadcasted_iota(jnp.int32, (row_count * 2, expert_count), 1)
    ).astype(jnp.int32)
    earlier = jnp.cumsum(onehot, axis=0) - onehot
    slot_index = jnp.sum(earlier * onehot, axis=1)
    target = flat_ids * capacity + slot_index
    placing = (
        target[None, :]
        == lax.broadcasted_iota(jnp.int32, (expert_count * capacity, row_count * 2), 0)
    ).astype(jnp.bfloat16)
    placing_tokens = jnp.sum(placing.reshape(expert_count * capacity, row_count, 2), axis=2)
    residual = project(expert_count, attended, out_weight, hidden_in)
    buffer = jnp.dot(placing_tokens, residual, preferred_element_type=jnp.float32).astype(
        jnp.bfloat16
    )
    returned = run_experts(
        chips,
        expert_count,
        buffer.reshape(expert_count, capacity, local_width),
        norm_gain.reshape(expert_count, 1, local_width),
        gate_proj.transpose(0, 2, 1),
        up_proj.transpose(0, 2, 1),
        down_proj,
    ).reshape(expert_count * capacity, local_width)
    gathered_back = lax.dot_general(
        placing, returned, (((0,), (0,)), ((), ())), preferred_element_type=jnp.float32
    )
    gathered_back = gathered_back.reshape(row_count, 2, local_width)
    combined = (
        residual.astype(jnp.float32)
        + gate_scale[:, 0:1] * gathered_back[:, 0]
        + gate_scale[:, 1:2] * gathered_back[:, 1]
    )
    return combined.astype(jnp.bfloat16)


def solution(mesh):
    placed = (
        P("ctx", "exp"),
        P("ctx", "exp"),
        P("ctx", "exp"),
        P("ctx", "exp"),
        P("exp", None),
        P(),
        P("exp", None, "ctx"),
        P("exp", None, "ctx"),
        P("exp", "ctx", None),
        P("ctx", None),
        P("ctx", None),
    )
    return jax.shard_map(
        local, mesh=mesh, in_specs=placed, out_specs=P("ctx", "exp"), check_vma=False
    )
```
